32 devices in a mesh: dom: 8 (over y, x, core), orb: 4 (over z).
Axes of the slice: x: 2, y: 2, z: 4, core: 2. Of those that a mesh axis runs over, the one named last changes fastest.
Arguments:
- orbitals: float32 [8, 64, 64, 128], P('orb', 'dom'), may hold values from -10.8 to 10.8
- initial_guess: float32 [8, 64, 64, 128], P('orb', 'dom'), may hold values from -350 to 350
- potential: float32 [64, 64, 128], P('dom'), may hold values from 0.1 to 2
- perturbation: float32 [64, 64, 128], P('dom'), may hold values from -6 to 6
- level_shifts: float32 [8], replicated, may hold values from 0.05 to 2
- assignment: int32 [8], P('orb'), may hold values from 0 to 7, each once
Outputs:
- updated_response: float32 [8, 64, 64, 128], P('orb', 'dom')
The draws below stay inside these ranges and needn't reach their ends.
Inputs may be any that keep to these rules, and one draw needn't show every extreme that they name: `assignment`: every energy index appears in exactly one slot.
All inputs are finite; a program needn't handle non-finite values.
Results may differ from the reference program's by a relative error of at most 0.0003.
Values sent between devices are 32-bit elements; how exact they have to be, the bound alone decides.
No kernel may reach another device: no remote copies, remote signals or barrier semaphores. Data moves between devices by JAX's collectives and lax.ppermute only.
A program may use at most 128 MiB of HBM per device.

```python
import math
import jax
import jax.numpy as jnp
from jax import lax

NY = 64
NZ = 128
SWEEPS = 2
COARSE = 4
NX = 64
ORBITALS = 8


def orbital_values(key):
    extent = (ORBITALS, NX, NY, NZ)
    sample = jnp.clip(jax.random.normal(jax.random.fold_in(key, 101), extent, jnp.float32), -6.0, 6.0)
    envelope = 0.6 + 1.2 * jnp.arange(NX, dtype=jnp.float32) / NX
    return sample * envelope[None, :, None, None]


def draw_orbitals(key, part):
    return orbital_values(key)


def draw_initial_guess(key, part):
    orbit_values = orbital_values(key)
    extent = (ORBITALS, NX, NY, NZ)
    coupling = 0.5 * jnp.clip(jax.random.normal(jax.random.fold_in(key, 202), (ORBITALS, ORBITALS), jnp.float32), -4.0, 4.0)
    jitter = jnp.clip(jax.random.normal(jax.random.fold_in(key, 303), extent, jnp.float32), -6.0, 6.0)
    blended = jnp.einsum('ji,jxyz->ixyz', coupling, orbit_values)
    return blended + 0.5 * jitter


def level_of(key, shape, shards, smallest, high):
    def one(position, parts):
        heights = jax.random.uniform(jax.random.fold_in(jax.random.fold_in(key, 6), position), (parts,), jnp.float32, smallest / len(shards), high / len(shards))
        return jnp.repeat(jnp.exp(heights), shape[position] // parts).reshape((-1,) + (1,) * (len(shape) - position - 1))

    gain = one(*shards[0])
    for cut in shards[1:]:
        gain = gain * one(*cut)
    return gain


def normal_values(stream_key, dims, spread, most, split=(), kind=jnp.bfloat16):
    drawn = spread * jax.random.normal(stream_key, dims, jnp.float32)
    if split:
        drawn = drawn * level_of(stream_key, dims, split, -0.22, 0.18)
    return jnp.clip(drawn, -most, most).astype(kind)


def setup_inputs(seed: int = 0) -> dict:
    seeds = jax.random.split(jax.random.key(seed), 7)
    return {
        "orbitals": draw_orbitals(jax.random.fold_in(seeds[6], 71), 0),
        "initial_guess": draw_initial_guess(jax.random.fold_in(seeds[6], 71), 0),
        "potential": jnp.clip(0.1 + 1.9 * jax.random.uniform(seeds[2], (NX, NY, NZ), jnp.float32) ** level_of(seeds[2], (NX, NY, NZ), ((0, 8),), -0.2, 0.2), 0.1, 2.0),
        "perturbation": normal_values(seeds[3], (NX, NY, NZ), 1.0, 6.0, ((0, 8),), jnp.float32),
        "level_shifts": jnp.clip(jnp.exp(jax.random.uniform(seeds[4], (ORBITALS,), jnp.float32, math.log(0.05), math.log(2.0))), 0.05, 2.0),
        "assignment": jax.random.permutation(seeds[5], ORBITALS).astype(jnp.int32),
    }


OMEGA = 0.8
KINETIC = 8.0


def apply_level(field_values, potential_level, shift_value, level):
    inverse_area = 0.25 ** level
    neighbours = (jnp.roll(field_values, -1, 0) + jnp.roll(field_values, 1, 0)) + (jnp.roll(field_values, -1, 1) + jnp.roll(field_values, 1, 1)) + (jnp.roll(field_values, -1, 2) + jnp.roll(field_values, 1, 2))
    return KINETIC * inverse_area * (6.0 * field_values - neighbours) + (potential_level + shift_value) * field_values


def diagonal_of(potential_level, shift_value, level):
    return 6.0 * KINETIC * 0.25 ** level + potential_level + shift_value


def relax(estimate, source, potential_level, shift_value, level):
    applied = apply_level(estimate, potential_level, shift_value, level)
    return estimate + OMEGA * (source - applied) / diagonal_of(potential_level, shift_value, level)


def coarsen(field_values):
    sx, sy, sz = field_values.shape
    return field_values.reshape(sx // 2, 2, sy // 2, 2, sz // 2, 2).mean(axis=(1, 3, 5))


def refine(field_values):
    return jnp.repeat(jnp.repeat(jnp.repeat(field_values, 2, 0), 2, 1), 2, 2)


def reference(orbitals, initial_guess, potential, perturbation, level_shifts, assignment):
    shifts = level_shifts[assignment.astype(jnp.int32)]
    levels = [potential]
    levels.append(coarsen(levels[0]))
    levels.append(coarsen(levels[1]))

    def solve_one(inputs):
        orbital, guess, shift_value = inputs
        source = -(perturbation * orbital)
        sources = [source - apply_level(guess, levels[0], shift_value, 0)]
        estimates = []
        for level in range(2):
            current = sources[level]
            estimate = OMEGA * current / diagonal_of(levels[level], shift_value, level)
            for sweep_index in range(SWEEPS - 1):
                estimate = relax(estimate, current, levels[level], shift_value, level)
            remainder = current - apply_level(estimate, levels[level], shift_value, level)
            estimates.append(estimate)
            sources.append(coarsen(remainder))
        lower = OMEGA * sources[2] / diagonal_of(levels[2], shift_value, 2)
        for sweep_index in range(COARSE - 1):
            lower = relax(lower, sources[2], levels[2], shift_value, 2)
        for level in (1, 0):
            estimate = estimates[level] + refine(lower)
            for sweep_index in range(SWEEPS):
                estimate = relax(estimate, sources[level], levels[level], shift_value, level)
            lower = estimate
        return guess + lower

    update = lax.map(solve_one, (orbitals, initial_guess, shifts))
    flat_orbit = orbitals.reshape(ORBITALS, -1)
    flat_update = update.reshape(ORBITALS, -1)
    intersection = jnp.einsum("jc,ic->ji", flat_orbit, flat_update, precision=lax.Precision.HIGHEST) / (NX * NY * NZ)
    result = flat_update - jnp.einsum("ji,jc->ic", intersection, flat_orbit, precision=lax.Precision.HIGHEST)
    return result.reshape(update.shape)
```

```python
import functools

import jax
import jax.numpy as jnp
from jax import lax
from jax.experimental import pallas as pl
from jax.experimental.pallas import tpu as pltpu
from jax.sharding import PartitionSpec as P

OMEGA = 0.8
KINETIC = 8.0
LANES = 128
REACH = 3


F32 = jnp.float32
VMEM = pl.BlockSpec(memory_space=pltpu.VMEM)
SMEM = pl.BlockSpec(memory_space=pltpu.SMEM)
ANY = pl.BlockSpec(memory_space=pl.ANY)


def roll(x, shift, axis):
    return pltpu.roll(x, shift % x.shape[axis], axis)


def around(x, group):
    y, z = x.ndim - 2, x.ndim - 1
    total = roll(x, 1, y) + roll(x, -1, y)
    if group == x.shape[z]:
        return total + (roll(x, 1, z) + roll(x, -1, z))
    place = lax.broadcasted_iota(jnp.int32, x.shape, z) % group
    before = jnp.where(place == 0, roll(x, 1 - group, z), roll(x, 1, z))
    after = jnp.where(place == group - 1, roll(x, group - 1, z), roll(x, -1, z))
    return total + (before + after)


def exact_dot(values, table):
    high = values.astype(jnp.bfloat16)
    rest = values - high.astype(F32)
    middle = rest.astype(jnp.bfloat16)
    low = (rest - middle.astype(F32)).astype(jnp.bfloat16)
    dot = functools.partial(jnp.dot, preferred_element_type=F32)
    return dot(high, table) + (dot(middle, table) + dot(low, table))


def pair_table(rows, columns, value):
    r = lax.broadcasted_iota(jnp.int32, (rows, columns), 0)
    c = lax.broadcasted_iota(jnp.int32, (rows, columns), 1)
    return jnp.where(r // 2 == c, value, 0.0).astype(jnp.bfloat16)


def spread_table(rows, columns):
    r = lax.broadcasted_iota(jnp.int32, (rows, columns), 0)
    c = lax.broadcasted_iota(jnp.int32, (rows, columns), 1)
    return jnp.where(c // 2 == r, 1.0, 0.0).astype(jnp.bfloat16)


def edge_kernel(shifts, assigned, guess, orbital, potential, perturbation, up, down, partial):
    count, depth = guess.shape[:2]
    for i in range(count):
        constant = 6.0 * KINETIC + shifts[assigned[i]]
        for x in range(depth):
            value = guess[i, x]
            near = around(value, LANES)
            if x > 0:
                near = near + guess[i, x - 1]
            if x < depth - 1:
                near = near + guess[i, x + 1]
            source = (
                KINETIC * near - (constant + potential[x]) * value - perturbation[x] * orbital[i, x]
            )
            partial[i, x] = source
            if x < REACH:
                down[(1 + x) * count + i] = source
            if x >= depth - REACH:
                up[(depth - x) * count + i] = source
        down[i] = guess[i, 0]
        up[i] = guess[i, depth - 1]
    for x in range(REACH):
        down[(1 + REACH) * count + x] = potential[x]
        up[(1 + REACH) * count + x] = potential[depth - 1 - x]


def fine_kernel(
    shifts, assigned, guess, partial, potential, low, high, estimate, scaled, weight, payload,
    all_scaled, all_weight, pairs,
):
    count, depth = guess.shape[:2]
    planes = depth + 2 * REACH
    first = (1 + REACH) * count

    def coefficient(p):
        x = p - REACH
        if x < 0:
            return low[first - 1 - x]
        if x >= depth:
            return high[first + x - depth]
        return potential[x]

    def source(i, p):
        x = p - REACH
        if x < 0:
            value = low[-x * count + i]
            return value + KINETIC * guess[i, 0] if x == -1 else value
        if x >= depth:
            value = high[(x - depth + 1) * count + i]
            return value + KINETIC * guess[i, depth - 1] if x == depth else value
        value = partial[i, x]
        if x == 0:
            value = value + KINETIC * low[i]
        if x == depth - 1:
            value = value + KINETIC * high[i]
        return value

    for i in range(count):
        constant = 6.0 * KINETIC + shifts[assigned[i]]
        for p in range(planes):
            w = OMEGA / (constant + coefficient(p))
            g = w * source(i, p)
            all_weight[i, p] = KINETIC * w
            all_scaled[i, p] = g
            if 2 <= p < planes - 2:
                scaled[i, p - 2] = g
                weight[i, p - 2] = KINETIC * w
    for i in range(count):
        for p in range(1, planes - 1):
            g = all_scaled[i, p]
            near = around(g, LANES) + (all_scaled[i, p - 1] + all_scaled[i, p + 1])
            estimate[i, p - 1] = (2.0 - OMEGA) * g + all_weight[i, p] * near
    half = depth // 2
    for i in range(count):
        constant = 6.0 * KINETIC + shifts[assigned[i]]
        for q in range(half):
            total = None
            for x in (2 * q, 2 * q + 1):
                e = estimate[i, x + 2]
                near = around(e, LANES) + (estimate[i, x + 1] + estimate[i, x + 3])
                r = (constant + potential[x]) * (
                    (1.0 / OMEGA) * all_scaled[i, x + REACH] - e
                ) + KINETIC * near
                total = r if total is None else total + r
            pairs[q * count + i] = total
    for q in range(half):
        pairs[half * count + q] = potential[2 * q] + potential[2 * q + 1]
    rows = pairs.shape[1] // 2
    slots = pairs.shape[0] // 2
    even = pairs[:, pl.ds(0, rows, 2), :] + pairs[:, pl.ds(1, rows, 2), :]
    even = even.reshape(slots, 2, rows, LANES)
    both = jnp.concatenate([even[:, 0], even[:, 1]], axis=-1).reshape(slots * rows, 2 * LANES)
    payload[...] = exact_dot(both, pair_table(2 * LANES, LANES, 0.125)).reshape(slots, rows, LANES)


def coarse_kernel(
    place, shifts, assigned, gathered, estimate, scaled, weight, guess, update,
    scaled1, weight1, coef1, e1, pairs, spread2, a1, b1, spread1, a0, b0,
):
    members = gathered.shape[0]
    count, depth = guess.shape[:2]
    half = depth // 2
    reach = 3
    window = (2 * reach + 1) * half
    rows1 = gathered.shape[2]
    group1 = LANES // count
    k1 = KINETIC / 4
    k2 = KINETIC / 16

    def shift_lanes(group):
        lane = lax.broadcasted_iota(jnp.int32, (1, 1, LANES), 2) // group
        value = jnp.full((1, 1, LANES), shifts[assigned[0]], F32)
        for i in range(1, count):
            value = jnp.where(lane % count == i, shifts[assigned[i]], value)
        return value

    base1 = 6.0 * k1 + shift_lanes(group1)
    base2 = 6.0 * k2 + shift_lanes(group1 // 2)
    lane = lax.broadcasted_iota(jnp.int32, (1, rows1, LANES), 2)
    for s in range(2 * reach + 1):
        slot = lax.rem(place[0] + (s - reach + 2 * members), members)
        f = gathered[slot, 0:half]
        for t in range(half // 2):
            packed = gathered[slot, half + t : half + t + 1]
            swapped = roll(packed, LANES // 2, 2)
            coef1[s * half + 2 * t : s * half + 2 * t + 1] = jnp.where(
                lane < LANES // 2, packed, swapped
            )
            coef1[s * half + 2 * t + 1 : s * half + 2 * t + 2] = jnp.where(
                lane < LANES // 2, swapped, packed
            )
        w = OMEGA / (base1 + coef1[s * half : (s + 1) * half])
        weight1[s * half : (s + 1) * half] = k1 * w
        scaled1[s * half : (s + 1) * half] = w * f
    step = 4
    for p in range(1, window - 1, step):
        stop = min(p + step, window - 1)
        g = scaled1[p:stop]
        near = around(g, group1) + (scaled1[p - 1 : stop - 1] + scaled1[p + 1 : stop + 1])
        e1[p:stop] = (2.0 - OMEGA) * g + weight1[p:stop] * near
    coarse = window // 2 - 2
    for p in range(2, window - 2, step):
        stop = min(p + step, window - 2)
        e = e1[p:stop]
        near = around(e, group1) + (e1[p - 1 : stop - 1] + e1[p + 1 : stop + 1])
        c = coef1[p:stop]
        r = (base1 + c) * ((1.0 / OMEGA) * scaled1[p:stop] - e) + k1 * near
        for t in range(0, stop - p, 2):
            pairs[(p + t) // 2 - 1] = r[t] + r[t + 1]
            pairs[coarse + (p + t) // 2 - 1] = c[t] + c[t + 1]
    rows2 = rows1 // 2
    even = pairs[:, pl.ds(0, rows2, 2), :] + pairs[:, pl.ds(1, rows2, 2), :]
    both = exact_dot(
        even.reshape(2 * coarse * rows2, LANES), pair_table(LANES, LANES, 0.125)
    ).reshape(2 * coarse, rows2, LANES)
    w = OMEGA / (base2 + both[coarse:])
    g = w * both[:coarse]
    w = k2 * w
    e = None
    for sweep in range(3):
        n = g.shape[0]
        if e is None:
            e = g
            mine = (2.0 - OMEGA) * g[1 : n - 1]
        else:
            mine = (1.0 - OMEGA) * e[1 : n - 1] + g[1 : n - 1]
        near = around(e[1 : n - 1], group1 // 2) + (e[0 : n - 2] + e[2:n])
        e = mine + w[1 : n - 1] * near
        g, w = g[1 : n - 1], w[1 : n - 1]
    n = e.shape[0]
    wide = exact_dot(e.reshape(n * rows2, LANES), spread_table(LANES, LANES))
    wide = wide.reshape(n, rows2, LANES)
    spread2[:, pl.ds(0, rows2, 2), :] = wide
    spread2[:, pl.ds(1, rows2, 2), :] = wide
    origin = reach * half
    for q in range(-3, half + 3):
        a1[q + 3] = e1[origin + q] + spread2[(q + 4) // 2]

    def sweep1(source, start, stop, offset):
        e = source[start - offset : stop - offset]
        near = around(e, group1) + (
            source[start - 1 - offset : stop - 1 - offset]
            + source[start + 1 - offset : stop + 1 - offset]
        )
        window = slice(origin + start, origin + stop)
        return (1.0 - OMEGA) * e + scaled1[window] + weight1[window] * near

    for q in range(-2, half + 2, 4):
        b1[q + 2 : q + 6] = sweep1(a1, q, q + 4, -3)
    last = sweep1(b1, -1, half + 1, -2)
    n = last.shape[0]
    wide = exact_dot(last.reshape(n * rows1, LANES), spread_table(LANES, count * LANES))
    wide = wide.reshape(n, rows1, count * LANES)
    for i in range(count):
        part = wide[:, :, i * LANES : (i + 1) * LANES]
        spread1[i, :, pl.ds(0, rows1, 2), :] = part
        spread1[i, :, pl.ds(1, rows1, 2), :] = part
    for i in range(count):
        for p in range(depth + 4):
            a0[i, p] = estimate[i, p] + spread1[i, p // 2]
    for i in range(count):
        for p in range(depth + 2):
            e = a0[i, p + 1]
            near = around(e, LANES) + (a0[i, p] + a0[i, p + 2])
            b0[i, p] = (1.0 - OMEGA) * e + scaled[i, p] + weight[i, p] * near
    for i in range(count):
        for p in range(depth):
            e = b0[i, p + 1]
            near = around(e, LANES) + (b0[i, p] + b0[i, p + 2])
            update[i, p] = guess[i, p] + (
                (1.0 - OMEGA) * e + scaled[i, p + 1] + weight[i, p + 1] * near
            )


def load_blocks(rank, blocks, buffer, sems, routes):
    for r, route in enumerate(routes):
        if len(route) == 1:
            pltpu.make_async_copy(blocks[route[0]], buffer.at[r], sems.at[r]).start()
            continue
        usual, other, where = route

        @pl.when(rank[0] == where)
        def _():
            pltpu.make_async_copy(blocks[other], buffer.at[r], sems.at[r]).start()

        @pl.when(rank[0] != where)
        def _():
            pltpu.make_async_copy(blocks[usual], buffer.at[r], sems.at[r]).start()


def wait_block(blocks, buffer, sems, r):
    pltpu.make_async_copy(blocks[0], buffer.at[r], sems.at[r]).wait()


def overlap_kernel(routes, blocks, rank, update, *refs):
    sources, (out, buffer, sems) = refs[:blocks], refs[blocks:]
    load_blocks(rank, sources, buffer, sems, routes)
    count, depth, rows = update.shape[:3]
    for r in range(len(routes)):
        wait_block(sources, buffer, sems, r)

        def body(x, totals, r=r):
            totals = list(totals)
            for j in range(count):
                o = buffer[r, j, x].reshape(rows // 8, 8, LANES)
                for i in range(count):
                    u = update[i, x].reshape(rows // 8, 8, LANES)
                    totals[j * count + i] += jnp.sum(o * u, axis=0)
            return tuple(totals)

        zero = jnp.zeros((8, LANES), F32)
        totals = lax.fori_loop(0, depth, body, (zero,) * (count * count))
        for k in range(count * count):
            out[r * count * count + k : r * count * count + k + 1] = jnp.sum(
                totals[k], axis=0, keepdims=True
            )


def project_kernel(routes, blocks, cells, rank, update, sums, *refs):
    sources, (out, buffer, sems) = refs[:blocks], refs[blocks:]
    load_blocks(rank, sources, buffer, sems, routes)
    count, depth, rows = update.shape[:3]
    total = sums[0]
    for m in range(1, sums.shape[0]):
        total = total + sums[m]
    overlap = jnp.sum(total, axis=1, keepdims=True) / cells
    for r in range(len(routes)):
        wait_block(sources, buffer, sems, r)

    def body(x, carry):
        for i in range(count):
            value = update[i, x]
            for r in range(len(routes)):
                for j in range(count):
                    k = (r * count + j) * count + i
                    value = value - overlap[k : k + 1] * buffer[r, j, x]
            out[i, x] = value
        return carry

    lax.fori_loop(0, depth, body, 0)


def gather_blocks(block, axis):
    n = lax.axis_size(axis)
    blocks, routes = [block], [(0,)]
    if n == 4:
        cross = lax.ppermute(block, axis, [(i, (i + 2) % n) for i in range(n)])
        above = lax.ppermute(block, axis, [(i + 1, i) for i in range(n - 1)])
        below = lax.ppermute(block, axis, [(i, i + 1) for i in range(n - 1)])
        far = lax.ppermute(cross, axis, [(2, 3), (1, 0)])
        return [block, above, cross, below, far], [(0,), (1, 4, n - 1), (2,), (3, 4, 0)]
    for r in range(1, n):
        blocks.append(lax.ppermute(block, axis, [((i + r) % n, i) for i in range(n)]))
        routes.append((r,))
    return blocks, routes


def on_device(orbitals, initial_guess, potential, perturbation, level_shifts, assignment):
    count, depth, ny, nz = orbitals.shape
    members = lax.axis_size("dom")
    half, rows1 = depth // 2, ny // 2
    assert nz == LANES and count * (nz // 2) == LANES and depth >= 2 * REACH
    plane = (ny, nz)
    shape = lambda *dims: jax.ShapeDtypeStruct(dims, F32)
    scratch = lambda *dims: pltpu.VMEM(dims, F32)
    params = pltpu.CompilerParams(vmem_limit_bytes=48 * 1024 * 1024)
    place = lax.axis_index("dom").astype(jnp.int32).reshape(1)
    rank = lax.axis_index("orb").astype(jnp.int32).reshape(1)

    blocks, routes = gather_blocks(orbitals, "orb")

    message = (1 + REACH) * count + REACH
    up, down, partial = pl.pallas_call(
        edge_kernel,
        out_shape=(shape(message, *plane), shape(message, *plane), shape(count, depth, *plane)),
        in_specs=[SMEM, SMEM] + [VMEM] * 4,
        out_specs=(VMEM,) * 3,
        compiler_params=params,
    )(level_shifts, assignment, initial_guess, orbitals, potential, perturbation)
    low = lax.ppermute(up, "dom", [(i, (i + 1) % members) for i in range(members)])
    high = lax.ppermute(down, "dom", [((i + 1) % members, i) for i in range(members)])

    estimate, scaled, weight, payload = pl.pallas_call(
        fine_kernel,
        out_shape=(
            shape(count, depth + 4, *plane),
            shape(count, depth + 2, *plane),
            shape(count, depth + 2, *plane),
            shape(half + half // 2, rows1, LANES),
        ),
        in_specs=[SMEM, SMEM] + [VMEM] * 5,
        out_specs=(VMEM,) * 4,
        scratch_shapes=[
            scratch(count, depth + 2 * REACH, *plane),
            scratch(count, depth + 2 * REACH, *plane),
            scratch(half * count + half, *plane),
        ],
        compiler_params=params,
    )(level_shifts, assignment, initial_guess, partial, potential, low, high)

    gathered = lax.all_gather(payload, "dom", axis=0)

    window = 7 * half
    update = pl.pallas_call(
        coarse_kernel,
        out_shape=shape(count, depth, *plane),
        in_specs=[SMEM, SMEM, SMEM] + [VMEM] * 5,
        out_specs=VMEM,
        scratch_shapes=[
            scratch(window, rows1, LANES),
            scratch(window, rows1, LANES),
            scratch(window, rows1, LANES),
            scratch(window, rows1, LANES),
            scratch(2 * (window // 2 - 2), rows1, LANES),
            scratch(6, rows1, LANES),
            scratch(half + 6, rows1, LANES),
            scratch(half + 4, rows1, LANES),
            scratch(count, half + 2, *plane),
            scratch(count, depth + 4, *plane),
            scratch(count, depth + 2, *plane),
        ],
        compiler_params=params,
    )(place, level_shifts, assignment, gathered, estimate, scaled, weight, initial_guess)

    pairs = len(routes) * count * count
    buffers = [
        scratch(len(routes), count, depth, *plane),
        pltpu.SemaphoreType.DMA((len(routes),)),
    ]
    sums = pl.pallas_call(
        functools.partial(overlap_kernel, routes, len(blocks)),
        out_shape=shape(pairs, LANES),
        in_specs=[SMEM, VMEM] + [ANY] * len(blocks),
        out_specs=VMEM,
        scratch_shapes=buffers,
        compiler_params=params,
    )(rank, update, *blocks)
    sums = lax.all_gather(sums, "dom", axis=0)
    cells = float(depth * members * ny * nz)
    return pl.pallas_call(
        functools.partial(project_kernel, routes, len(blocks), cells),
        out_shape=shape(count, depth, *plane),
        in_specs=[SMEM, VMEM, VMEM] + [ANY] * len(blocks),
        out_specs=VMEM,
        scratch_shapes=buffers,
        compiler_params=params,
    )(rank, update, sums, *blocks)


def solution(mesh):
    in_specs = (
        P("orb", "dom", None, None),
        P("orb", "dom", None, None),
        P("dom", None, None),
        P("dom", None, None),
        P(),
        P("orb"),
    )
    return jax.shard_map(
        on_device,
        mesh=mesh,
        in_specs=in_specs,
        out_specs=P("orb", "dom", None, None),
        check_vma=False,
    )
```

```python
import functools

import jax
import jax.numpy as jnp
from jax import lax
from jax.experimental import pallas as pl
from jax.experimental.pallas import tpu as pltpu
from jax.sharding import PartitionSpec as P


OMEGA = 0.8
KINETIC = 8.0
LANES = 128
REACH = 3


F32 = jnp.float32
VMEM = pl.BlockSpec(memory_space=pltpu.VMEM)
SMEM = pl.BlockSpec(memory_space=pltpu.SMEM)
HBM = pl.BlockSpec(memory_space=pltpu.HBM)


def roll(x, shift, axis):
    return pltpu.roll(x, shift % x.shape[axis], axis)


def around(x, group):
    y, z = x.ndim - 2, x.ndim - 1
    total = roll(x, 1, y) + roll(x, -1, y)
    if group == x.shape[z]:
        return total + (roll(x, 1, z) + roll(x, -1, z))
    place = lax.broadcasted_iota(jnp.int32, x.shape, z) % group
    before = jnp.where(place == 0, roll(x, 1 - group, z), roll(x, 1, z))
    after = jnp.where(place == group - 1, roll(x, group - 1, z), roll(x, -1, z))
    return total + (before + after)


def exact_dot(values, table):
    high = values.astype(jnp.bfloat16)
    rest = values - high.astype(F32)
    middle = rest.astype(jnp.bfloat16)
    low = (rest - middle.astype(F32)).astype(jnp.bfloat16)
    dot = functools.partial(jnp.dot, preferred_element_type=F32)
    return dot(high, table) + (dot(middle, table) + dot(low, table))


def pair_table(rows, columns, value):
    r = lax.broadcasted_iota(jnp.int32, (rows, columns), 0)
    c = lax.broadcasted_iota(jnp.int32, (rows, columns), 1)
    return jnp.where(r // 2 == c, value, 0.0).astype(jnp.bfloat16)


def spread_table(rows, columns):
    r = lax.broadcasted_iota(jnp.int32, (rows, columns), 0)
    c = lax.broadcasted_iota(jnp.int32, (rows, columns), 1)
    return jnp.where(c // 2 == r, 1.0, 0.0).astype(jnp.bfloat16)


def load_all(pairs, sems):
    copies = [
        pltpu.make_async_copy(source, target, sems.at[k]) for k, (source, target) in enumerate(pairs)
    ]
    for copy in copies:
        copy.start()
    for copy in copies:
        copy.wait()


def own_source(i, x, constant, guess, orbital, potential, perturbation):
    value = guess[i, x]
    near = around(value, LANES)
    if x > 0:
        near = near + guess[i, x - 1]
    if x < guess.shape[1] - 1:
        near = near + guess[i, x + 1]
    return KINETIC * near - (constant + potential[x]) * value - perturbation[x] * orbital[i, x]


def edge_kernel(
    shifts_in, assigned_in, guess_in, orbital_in, potential_in, perturbation_in, up, down,
    shifts, assigned, guess, orbital, potential, perturbation, sems,
):
    fields = (guess, orbital, potential, perturbation)
    inputs = (shifts_in, assigned_in, guess_in, orbital_in, potential_in, perturbation_in)
    load_all(zip(inputs, (shifts, assigned) + fields), sems)
    count, depth = guess.shape[:2]
    for i in range(count):
        constant = 6.0 * KINETIC + shifts[assigned[i]]
        down[i] = guess[i, 0]
        up[i] = guess[i, depth - 1]
        for x in range(REACH):
            down[(1 + x) * count + i] = own_source(i, x, constant, *fields)
            up[(1 + x) * count + i] = own_source(i, depth - 1 - x, constant, *fields)
    for x in range(REACH):
        down[(1 + REACH) * count + x] = potential[x]
        up[(1 + REACH) * count + x] = potential[depth - 1 - x]


def own_kernel(
    shifts_in, assigned_in, guess_in, orbital_in, potential_in, perturbation_in, scaled, weight,
    shifts, assigned, guess, orbital, potential, perturbation, sems,
):
    fields = (guess, orbital, potential, perturbation)
    inputs = (shifts_in, assigned_in, guess_in, orbital_in, potential_in, perturbation_in)
    load_all(zip(inputs, (shifts, assigned) + fields), sems)
    count, depth = guess.shape[:2]
    for i in range(count):
        constant = 6.0 * KINETIC + shifts[assigned[i]]
        for x in range(depth):
            w = OMEGA / (constant + potential[x])
            weight[i, x] = KINETIC * w
            scaled[i, x] = w * own_source(i, x, constant, *fields)


def fine_kernel(
    shifts, assigned, own_scaled, own_weight, potential, low, high, up, down, estimate, scaled, weight, payload,
    all_scaled, all_weight, pairs,
):
    count, depth = own_scaled.shape[:2]
    planes = depth + 2 * REACH
    first = (1 + REACH) * count

    for i in range(count):
        constant = 6.0 * KINETIC + shifts[assigned[i]]
        for p in range(planes):
            x = p - REACH
            if 0 <= x < depth:
                kw = own_weight[i, x]
                g = own_scaled[i, x]
                if x == 0:
                    g = g + kw * low[i]
                if x == depth - 1:
                    g = g + kw * high[i]
            else:
                side, away = (low, -1 - x) if x < 0 else (high, x - depth)
                w = OMEGA / (constant + side[first + away])
                kw = KINETIC * w
                g = w * side[(1 + away) * count + i]
                if away == 0:
                    g = g + kw * (down if x < 0 else up)[i]
            all_weight[i, p] = kw
            all_scaled[i, p] = g
            if 2 <= p < planes - 2:
                scaled[i, p - 2] = g
                weight[i, p - 2] = kw
    for i in range(count):
        for p in range(1, planes - 1):
            g = all_scaled[i, p]
            near = around(g, LANES) + (all_scaled[i, p - 1] + all_scaled[i, p + 1])
            estimate[i, p - 1] = (2.0 - OMEGA) * g + all_weight[i, p] * near
    half = depth // 2
    for i in range(count):
        constant = 6.0 * KINETIC + shifts[assigned[i]]
        for q in range(half):
            total = None
            for x in (2 * q, 2 * q + 1):
                e = estimate[i, x + 2]
                near = around(e, LANES) + (estimate[i, x + 1] + estimate[i, x + 3])
                r = (constant + potential[x]) * (
                    (1.0 / OMEGA) * all_scaled[i, x + REACH] - e
                ) + KINETIC * near
                total = r if total is None else total + r
            pairs[q * count + i] = total
    for q in range(half):
        pairs[half * count + q] = potential[2 * q] + potential[2 * q + 1]
    rows = pairs.shape[1] // 2
    slots = pairs.shape[0] // 2
    even = pairs[:, pl.ds(0, rows, 2), :] + pairs[:, pl.ds(1, rows, 2), :]
    even = even.reshape(slots, 2, rows, LANES)
    both = jnp.concatenate([even[:, 0], even[:, 1]], axis=-1).reshape(slots * rows, 2 * LANES)
    payload[...] = exact_dot(both, pair_table(2 * LANES, LANES, 0.125)).reshape(slots, rows, LANES)


def coarse_kernel(
    place, shifts, assigned, gathered, estimate, scaled, weight, guess, update,
    scaled1, weight1, coef1, e1, pairs, spread2, a1, b1, spread1, a0, b0,
):
    members = gathered.shape[0]
    count, depth = guess.shape[:2]
    half = depth // 2
    reach = 3
    window = (2 * reach + 1) * half
    rows1 = gathered.shape[2]
    group1 = LANES // count
    k1 = KINETIC / 4
    k2 = KINETIC / 16

    def shift_lanes(group):
        lane = lax.broadcasted_iota(jnp.int32, (1, 1, LANES), 2) // group
        value = jnp.full((1, 1, LANES), shifts[assigned[0]], F32)
        for i in range(1, count):
            value = jnp.where(lane % count == i, shifts[assigned[i]], value)
        return value

    base1 = 6.0 * k1 + shift_lanes(group1)
    base2 = 6.0 * k2 + shift_lanes(group1 // 2)
    lane = lax.broadcasted_iota(jnp.int32, (1, rows1, LANES), 2)
    for s in range(2 * reach + 1):
        slot = lax.rem(place[0] + (s - reach + 2 * members), members)
        f = gathered[slot, 0:half]
        for t in range(half // 2):
            packed = gathered[slot, half + t : half + t + 1]
            swapped = roll(packed, LANES // 2, 2)
            coef1[s * half + 2 * t : s * half + 2 * t + 1] = jnp.where(
                lane < LANES // 2, packed, swapped
            )
            coef1[s * half + 2 * t + 1 : s * half + 2 * t + 2] = jnp.where(
                lane < LANES // 2, swapped, packed
            )
        w = OMEGA / (base1 + coef1[s * half : (s + 1) * half])
        weight1[s * half : (s + 1) * half] = k1 * w
        scaled1[s * half : (s + 1) * half] = w * f
    step = 4
    for p in range(1, window - 1, step):
        stop = min(p + step, window - 1)
        g = scaled1[p:stop]
        near = around(g, group1) + (scaled1[p - 1 : stop - 1] + scaled1[p + 1 : stop + 1])
        e1[p:stop] = (2.0 - OMEGA) * g + weight1[p:stop] * near
    coarse = window // 2 - 2
    for p in range(2, window - 2, step):
        stop = min(p + step, window - 2)
        e = e1[p:stop]
        near = around(e, group1) + (e1[p - 1 : stop - 1] + e1[p + 1 : stop + 1])
        c = coef1[p:stop]
        r = (base1 + c) * ((1.0 / OMEGA) * scaled1[p:stop] - e) + k1 * near
        for t in range(0, stop - p, 2):
            pairs[(p + t) // 2 - 1] = r[t] + r[t + 1]
            pairs[coarse + (p + t) // 2 - 1] = c[t] + c[t + 1]
    rows2 = rows1 // 2
    even = pairs[:, pl.ds(0, rows2, 2), :] + pairs[:, pl.ds(1, rows2, 2), :]
    both = exact_dot(
        even.reshape(2 * coarse * rows2, LANES), pair_table(LANES, LANES, 0.125)
    ).reshape(2 * coarse, rows2, LANES)
    w = OMEGA / (base2 + both[coarse:])
    g = w * both[:coarse]
    w = k2 * w
    e = None
    for _ in range(3):
        n = g.shape[0]
        if e is None:
            e = g
            mine = (2.0 - OMEGA) * g[1 : n - 1]
        else:
            mine = (1.0 - OMEGA) * e[1 : n - 1] + g[1 : n - 1]
        near = around(e[1 : n - 1], group1 // 2) + (e[0 : n - 2] + e[2:n])
        e = mine + w[1 : n - 1] * near
        g, w = g[1 : n - 1], w[1 : n - 1]
    n = e.shape[0]
    wide = exact_dot(e.reshape(n * rows2, LANES), spread_table(LANES, LANES))
    wide = wide.reshape(n, rows2, LANES)
    spread2[:, pl.ds(0, rows2, 2), :] = wide
    spread2[:, pl.ds(1, rows2, 2), :] = wide
    origin = reach * half
    for q in range(-3, half + 3):
        a1[q + 3] = e1[origin + q] + spread2[(q + 4) // 2]

    def sweep1(source, start, stop, offset):
        e = source[start - offset : stop - offset]
        near = around(e, group1) + (
            source[start - 1 - offset : stop - 1 - offset]
            + source[start + 1 - offset : stop + 1 - offset]
        )
        window = slice(origin + start, origin + stop)
        return (1.0 - OMEGA) * e + scaled1[window] + weight1[window] * near

    for q in range(-2, half + 2, 4):
        b1[q + 2 : q + 6] = sweep1(a1, q, q + 4, -3)
    last = sweep1(b1, -1, half + 1, -2)
    n = last.shape[0]
    wide = exact_dot(last.reshape(n * rows1, LANES), spread_table(LANES, count * LANES))
    wide = wide.reshape(n, rows1, count * LANES)
    for i in range(count):
        part = wide[:, :, i * LANES : (i + 1) * LANES]
        spread1[i, :, pl.ds(0, rows1, 2), :] = part
        spread1[i, :, pl.ds(1, rows1, 2), :] = part
    for i in range(count):
        for p in range(depth + 4):
            a0[i, p] = estimate[i, p] + spread1[i, p // 2]
    for i in range(count):
        for p in range(depth + 2):
            e = a0[i, p + 1]
            near = around(e, LANES) + (a0[i, p] + a0[i, p + 2])
            b0[i, p] = (1.0 - OMEGA) * e + scaled[i, p] + weight[i, p] * near
    for i in range(count):
        for p in range(depth):
            e = b0[i, p + 1]
            near = around(e, LANES) + (b0[i, p] + b0[i, p + 2])
            update[i, p] = guess[i, p] + (
                (1.0 - OMEGA) * e + scaled[i, p + 1] + weight[i, p + 1] * near
            )


def row_sums(blocks, update, out, first):
    count, depth, rows = update.shape[:3]

    def body(x, totals):
        totals = list(totals)
        u = [update[i, x].reshape(rows // 8, 8, LANES) for i in range(count)]
        for r, block in enumerate(blocks):
            for j in range(count):
                o = block(j, x).reshape(rows // 8, 8, LANES)
                for i in range(count):
                    totals[(r * count + j) * count + i] += jnp.sum(o * u[i], axis=0)
        return tuple(totals)

    zero = jnp.zeros((8, LANES), F32)
    totals = lax.fori_loop(0, depth, body, (zero,) * (len(blocks) * count * count))
    for k, total in enumerate(totals):
        out[first + k : first + k + 1] = jnp.sum(total, axis=0, keepdims=True)


def reader(*refs):
    def read(j, x):
        value = refs[0][j, x]
        for ref in refs[1:]:
            value = value + ref[j, x]
        return value

    return read


def early_kernel(blocks, update, own_in, *refs):
    others, (out, own, sem) = refs[:blocks], refs[blocks:]
    copy = pltpu.make_async_copy(own_in, own, sem)
    copy.start()
    copy.wait()
    row_sums([reader(own)] + [reader(other) for other in others], update, out, 0)


def late_kernel(update, early, *refs):
    last, out = refs[:-1], refs[-1]
    rows = early.shape[0]
    out[0:rows] = early[...]
    row_sums([reader(*last)], update, out, rows)


def project_kernel(blocks, parts, cells, update, own_in, *refs):
    others, last = refs[:blocks], refs[blocks:-3 - parts]
    sums, (out, own, sem) = refs[-3 - parts : -3], refs[-3:]
    copy = pltpu.make_async_copy(own_in, own, sem)
    copy.start()
    count, depth, _ = update.shape[:3]
    total = sums[0][...]
    for part in sums[1:]:
        total = total + part[...]
    overlap = jnp.sum(total, axis=1, keepdims=True) / cells
    copy.wait()
    reads = [reader(own)] + [reader(other) for other in others] + [reader(*last)]

    def body(x, carry):
        values = [update[i, x] for i in range(count)]
        for r, read in enumerate(reads):
            for j in range(count):
                o = read(j, x)
                for i in range(count):
                    k = (r * count + j) * count + i
                    values[i] = values[i] - overlap[k : k + 1] * o
        for i in range(count):
            out[i, x] = values[i]
        return carry

    lax.fori_loop(0, depth, body, 0)


def gather_blocks(block, axis):
    n = lax.axis_size(axis)
    if n == 4:
        first = lax.ppermute(block, axis, [(0, 2), (3, 1), (2, 3), (1, 0)])
        second = lax.ppermute(block, axis, [(1, 3), (2, 0), (0, 1), (3, 2)])
        inner = lax.ppermute(block, axis, [(1, 2), (2, 1)])
        outer = lax.ppermute(first, axis, [(2, 3), (1, 0)])
        return [first, second], [inner, outer]
    blocks = []
    for r in range(1, n):
        blocks.append(lax.ppermute(block, axis, [((i + r) % n, i) for i in range(n)]))
    return blocks[:-1], blocks[-1:]


def reduce_parts(value, axis):
    n = lax.axis_size(axis)
    if n & (n - 1):
        return [lax.psum(value, axis)]
    parts, stride, width = [value], 1, 2
    while stride < n:
        total = parts[0]
        for part in parts[1:]:
            total = total + part
        width = min(width, n // stride)
        parts = [total] + [
            lax.ppermute(total, axis, [(i, i ^ (k * stride)) for i in range(n)])
            for k in range(width - 1, 0, -1)
        ]
        stride, width = stride * width, 4
    return parts


def on_device(orbitals, initial_guess, potential, perturbation, level_shifts, assignment):
    count, depth, ny, nz = orbitals.shape
    near = lambda x: pltpu.with_memory_space_constraint(x, pltpu.HBM)
    members = lax.axis_size("dom")
    half, rows1 = depth // 2, ny // 2
    assert nz == LANES and count * (nz // 2) == LANES and depth >= 2 * REACH
    plane = (ny, nz)
    shape = lambda *dims: jax.ShapeDtypeStruct(dims, F32)
    scratch = lambda *dims: pltpu.VMEM(dims, F32)
    params = pltpu.CompilerParams(vmem_limit_bytes=24 * 1024 * 1024)
    place = lax.axis_index("dom").astype(jnp.int32).reshape(1)

    blocks, last = gather_blocks(orbitals, "orb")

    message = (1 + REACH) * count + REACH
    inputs = tuple(
        map(near, (level_shifts, assignment, initial_guess, orbitals, potential, perturbation))
    )
    local = [
        pltpu.SMEM(level_shifts.shape, F32),
        pltpu.SMEM(assignment.shape, jnp.int32),
        scratch(count, depth, *plane),
        scratch(count, depth, *plane),
        scratch(depth, *plane),
        scratch(depth, *plane),
        pltpu.SemaphoreType.DMA((6,)),
    ]
    up, down = pl.pallas_call(
        edge_kernel,
        out_shape=(shape(message, *plane),) * 2,
        in_specs=[HBM] * 6,
        out_specs=(VMEM,) * 2,
        scratch_shapes=local,
        compiler_params=params,
    )(*inputs)
    own_scaled, own_weight = pl.pallas_call(
        own_kernel,
        out_shape=(shape(count, depth, *plane),) * 2,
        in_specs=[HBM] * 6,
        out_specs=(VMEM,) * 2,
        scratch_shapes=local,
        compiler_params=params,
    )(*inputs)
    low = lax.ppermute(up, "dom", [(i, (i + 1) % members) for i in range(members)])
    high = lax.ppermute(down, "dom", [((i + 1) % members, i) for i in range(members)])

    estimate, scaled, weight, payload = pl.pallas_call(
        fine_kernel,
        out_shape=(
            shape(count, depth + 4, *plane),
            shape(count, depth + 2, *plane),
            shape(count, depth + 2, *plane),
            shape(half + half // 2, rows1, LANES),
        ),
        in_specs=[SMEM, SMEM] + [VMEM] * 7,
        out_specs=(VMEM,) * 4,
        scratch_shapes=[
            scratch(count, depth + 2 * REACH, *plane),
            scratch(count, depth + 2 * REACH, *plane),
            scratch(half * count + half, *plane),
        ],
        compiler_params=params,
    )(level_shifts, assignment, near(own_scaled), near(own_weight), potential, low, high, up, down)

    gathered = lax.all_gather(payload, "dom", axis=0)

    window = 7 * half
    update = pl.pallas_call(
        coarse_kernel,
        out_shape=shape(count, depth, *plane),
        in_specs=[SMEM, SMEM, SMEM] + [VMEM] * 5,
        out_specs=VMEM,
        scratch_shapes=[
            scratch(window, rows1, LANES),
            scratch(window, rows1, LANES),
            scratch(window, rows1, LANES),
            scratch(window, rows1, LANES),
            scratch(2 * (window // 2 - 2), rows1, LANES),
            scratch(6, rows1, LANES),
            scratch(half + 6, rows1, LANES),
            scratch(half + 4, rows1, LANES),
            scratch(count, half + 2, *plane),
            scratch(count, depth + 4, *plane),
            scratch(count, depth + 2, *plane),
        ],
        compiler_params=params,
    )(place, level_shifts, assignment, gathered, estimate, scaled, weight, initial_guess)

    own = [scratch(count, depth, *plane), pltpu.SemaphoreType.DMA(())]
    rows = (1 + len(blocks)) * count * count
    sums = pl.pallas_call(
        functools.partial(early_kernel, len(blocks)),
        out_shape=shape(rows, LANES),
        in_specs=[VMEM, HBM] + [VMEM] * len(blocks),
        out_specs=VMEM,
        scratch_shapes=own,
        compiler_params=params,
    )(update, orbitals, *blocks)
    sums = pl.pallas_call(
        late_kernel,
        out_shape=shape(rows + count * count, LANES),
        in_specs=[VMEM] * (2 + len(last)),
        out_specs=VMEM,
        compiler_params=params,
    )(update, sums, *last)
    parts = reduce_parts(sums, "dom")
    cells = float(depth * members * ny * nz)
    return pl.pallas_call(
        functools.partial(project_kernel, len(blocks), len(parts), cells),
        out_shape=shape(count, depth, *plane),
        in_specs=[VMEM, HBM] + [VMEM] * (len(blocks) + len(last) + len(parts)),
        out_specs=VMEM,
        scratch_shapes=own,
        compiler_params=params,
    )(update, orbitals, *blocks, *last, *parts)


def solution(mesh):
    in_specs = (
        P("orb", "dom", None, None),
        P("orb", "dom", None, None),
        P("dom", None, None),
        P("dom", None, None),
        P(),
        P("orb"),
    )
    return jax.shard_map(
        on_device,
        mesh=mesh,
        in_specs=in_specs,
        out_specs=P("orb", "dom", None, None),
        check_vma=False,
    )
```

```python
import functools

import jax
import jax.numpy as jnp
from jax import lax
from jax.experimental import pallas as pl
from jax.experimental.pallas import tpu as pltpu
from jax.sharding import PartitionSpec as P


OMEGA = 0.8
KINETIC = 8.0
LANES = 128
REACH = 3


F32 = jnp.float32
VMEM = pl.BlockSpec(memory_space=pltpu.VMEM)
SMEM = pl.BlockSpec(memory_space=pltpu.SMEM)
HBM = pl.BlockSpec(memory_space=pltpu.HBM)


def roll(x, shift, axis):
    return pltpu.roll(x, shift % x.shape[axis], axis)


def around(x, group):
    y, z = x.ndim - 2, x.ndim - 1
    total = roll(x, 1, y) + roll(x, -1, y)
    if group == x.shape[z]:
        return total + (roll(x, 1, z) + roll(x, -1, z))
    place = lax.broadcasted_iota(jnp.int32, x.shape, z) % group
    before = jnp.where(place == 0, roll(x, 1 - group, z), roll(x, 1, z))
    after = jnp.where(place == group - 1, roll(x, group - 1, z), roll(x, -1, z))
    return total + (before + after)


def exact_dot(values, table):
    high = values.astype(jnp.bfloat16)
    rest = values - high.astype(F32)
    middle = rest.astype(jnp.bfloat16)
    low = (rest - middle.astype(F32)).astype(jnp.bfloat16)
    dot = functools.partial(jnp.dot, preferred_element_type=F32)
    return dot(high, table) + (dot(middle, table) + dot(low, table))


def pair_table(rows, columns, value):
    r = lax.broadcasted_iota(jnp.int32, (rows, columns), 0)
    c = lax.broadcasted_iota(jnp.int32, (rows, columns), 1)
    return jnp.where(r // 2 == c, value, 0.0).astype(jnp.bfloat16)


def spread_table(rows, columns):
    r = lax.broadcasted_iota(jnp.int32, (rows, columns), 0)
    c = lax.broadcasted_iota(jnp.int32, (rows, columns), 1)
    return jnp.where(c // 2 == r, 1.0, 0.0).astype(jnp.bfloat16)


def load_all(pairs, sems):
    copies = [
        pltpu.make_async_copy(source, target, sems.at[k]) for k, (source, target) in enumerate(pairs)
    ]
    for copy in copies:
        copy.start()
    for copy in copies:
        copy.wait()


def own_source(i, x, constant, guess, orbital, potential, perturbation):
    value = guess[i, x]
    near = around(value, LANES)
    if x > 0:
        near = near + guess[i, x - 1]
    if x < guess.shape[1] - 1:
        near = near + guess[i, x + 1]
    return KINETIC * near - (constant + potential[x]) * value - perturbation[x] * orbital[i, x]


def edge_kernel(
    shifts_in, assigned_in, guess_in, orbital_in, potential_in, perturbation_in, up, down,
    shifts, assigned, guess, orbital, potential, perturbation, sems,
):
    fields = (guess, orbital, potential, perturbation)
    inputs = (shifts_in, assigned_in, guess_in, orbital_in, potential_in, perturbation_in)
    load_all(zip(inputs, (shifts, assigned) + fields), sems)
    count, depth = guess.shape[:2]
    for i in range(count):
        constant = 6.0 * KINETIC + shifts[assigned[i]]
        down[i] = guess[i, 0]
        up[i] = guess[i, depth - 1]
        for x in range(REACH):
            down[(1 + x) * count + i] = own_source(i, x, constant, *fields)
            up[(1 + x) * count + i] = own_source(i, depth - 1 - x, constant, *fields)
    for x in range(REACH):
        down[(1 + REACH) * count + x] = potential[x]
        up[(1 + REACH) * count + x] = potential[depth - 1 - x]


def own_kernel(
    shifts_in, assigned_in, guess_in, orbital_in, potential_in, perturbation_in, scaled, weight,
    shifts, assigned, guess, orbital, potential, perturbation, sems,
):
    fields = (guess, orbital, potential, perturbation)
    inputs = (shifts_in, assigned_in, guess_in, orbital_in, potential_in, perturbation_in)
    load_all(zip(inputs, (shifts, assigned) + fields), sems)
    count, depth = guess.shape[:2]
    for i in range(count):
        constant = 6.0 * KINETIC + shifts[assigned[i]]
        for x in range(depth):
            w = OMEGA / (constant + potential[x])
            weight[i, x] = KINETIC * w
            scaled[i, x] = w * own_source(i, x, constant, *fields)


def fine_kernel(
    shifts, assigned, own_scaled, own_weight, potential, low, high, up, down, estimate, scaled, weight, payload,
    all_scaled, all_weight, pairs,
):
    count, depth = own_scaled.shape[:2]
    planes = depth + 2 * REACH
    first = (1 + REACH) * count

    for i in range(count):
        constant = 6.0 * KINETIC + shifts[assigned[i]]
        for p in range(planes):
            x = p - REACH
            if 0 <= x < depth:
                kw = own_weight[i, x]
                g = own_scaled[i, x]
                if x == 0:
                    g = g + kw * low[i]
                if x == depth - 1:
                    g = g + kw * high[i]
            else:
                side, away = (low, -1 - x) if x < 0 else (high, x - depth)
                w = OMEGA / (constant + side[first + away])
                kw = KINETIC * w
                g = w * side[(1 + away) * count + i]
                if away == 0:
                    g = g + kw * (down if x < 0 else up)[i]
            all_weight[i, p] = kw
            all_scaled[i, p] = g
            if 2 <= p < planes - 2:
                scaled[i, p - 2] = g
                weight[i, p - 2] = kw
    for i in range(count):
        for p in range(1, planes - 1):
            g = all_scaled[i, p]
            near = around(g, LANES) + (all_scaled[i, p - 1] + all_scaled[i, p + 1])
            estimate[i, p - 1] = (2.0 - OMEGA) * g + all_weight[i, p] * near
    half = depth // 2
    for i in range(count):
        constant = 6.0 * KINETIC + shifts[assigned[i]]
        for q in range(half):
            total = None
            for x in (2 * q, 2 * q + 1):
                e = estimate[i, x + 2]
                near = around(e, LANES) + (estimate[i, x + 1] + estimate[i, x + 3])
                r = (constant + potential[x]) * (
                    (1.0 / OMEGA) * all_scaled[i, x + REACH] - e
                ) + KINETIC * near
                total = r if total is None else total + r
            pairs[q * count + i] = total
    for q in range(half):
        pairs[half * count + q] = potential[2 * q] + potential[2 * q + 1]
    rows = pairs.shape[1] // 2
    slots = pairs.shape[0] // 2
    even = pairs[:, pl.ds(0, rows, 2), :] + pairs[:, pl.ds(1, rows, 2), :]
    even = even.reshape(slots, 2, rows, LANES)
    both = jnp.concatenate([even[:, 0], even[:, 1]], axis=-1).reshape(slots * rows, 2 * LANES)
    payload[...] = exact_dot(both, pair_table(2 * LANES, LANES, 0.125)).reshape(slots, rows, LANES)


def coarse_kernel(
    place, shifts, assigned, gathered, estimate, scaled, weight, guess, update,
    scaled1, weight1, coef1, e1, pairs, spread2, a1, b1, spread1, a0, b0,
):
    members = gathered.shape[0]
    count, depth = guess.shape[:2]
    half = depth // 2
    reach = 3
    window = (2 * reach + 1) * half
    rows1 = gathered.shape[2]
    group1 = LANES // count
    k1 = KINETIC / 4
    k2 = KINETIC / 16

    def shift_lanes(group):
        lane = lax.broadcasted_iota(jnp.int32, (1, 1, LANES), 2) // group
        value = jnp.full((1, 1, LANES), shifts[assigned[0]], F32)
        for i in range(1, count):
            value = jnp.where(lane % count == i, shifts[assigned[i]], value)
        return value

    base1 = 6.0 * k1 + shift_lanes(group1)
    base2 = 6.0 * k2 + shift_lanes(group1 // 2)
    lane = lax.broadcasted_iota(jnp.int32, (1, rows1, LANES), 2)
    for s in range(2 * reach + 1):
        slot = lax.rem(place[0] + (s - reach + 2 * members), members)
        f = gathered[slot, 0:half]
        for t in range(half // 2):
            packed = gathered[slot, half + t : half + t + 1]
            swapped = roll(packed, LANES // 2, 2)
            coef1[s * half + 2 * t : s * half + 2 * t + 1] = jnp.where(
                lane < LANES // 2, packed, swapped
            )
            coef1[s * half + 2 * t + 1 : s * half + 2 * t + 2] = jnp.where(
                lane < LANES // 2, swapped, packed
            )
        w = OMEGA / (base1 + coef1[s * half : (s + 1) * half])
        weight1[s * half : (s + 1) * half] = k1 * w
        scaled1[s * half : (s + 1) * half] = w * f
    step = 4
    for p in range(1, window - 1, step):
        stop = min(p + step, window - 1)
        g = scaled1[p:stop]
        near = around(g, group1) + (scaled1[p - 1 : stop - 1] + scaled1[p + 1 : stop + 1])
        e1[p:stop] = (2.0 - OMEGA) * g + weight1[p:stop] * near
    coarse = window // 2 - 2
    for p in range(2, window - 2, step):
        stop = min(p + step, window - 2)
        e = e1[p:stop]
        near = around(e, group1) + (e1[p - 1 : stop - 1] + e1[p + 1 : stop + 1])
        c = coef1[p:stop]
        r = (base1 + c) * ((1.0 / OMEGA) * scaled1[p:stop] - e) + k1 * near
        for t in range(0, stop - p, 2):
            pairs[(p + t) // 2 - 1] = r[t] + r[t + 1]
            pairs[coarse + (p + t) // 2 - 1] = c[t] + c[t + 1]
    rows2 = rows1 // 2
    even = pairs[:, pl.ds(0, rows2, 2), :] + pairs[:, pl.ds(1, rows2, 2), :]
    both = exact_dot(
        even.reshape(2 * coarse * rows2, LANES), pair_table(LANES, LANES, 0.125)
    ).reshape(2 * coarse, rows2, LANES)
    w = OMEGA / (base2 + both[coarse:])
    g = w * both[:coarse]
    w = k2 * w
    e = None
    for _ in range(3):
        n = g.shape[0]
        if e is None:
            e = g
            mine = (2.0 - OMEGA) * g[1 : n - 1]
        else:
            mine = (1.0 - OMEGA) * e[1 : n - 1] + g[1 : n - 1]
        near = around(e[1 : n - 1], group1 // 2) + (e[0 : n - 2] + e[2:n])
        e = mine + w[1 : n - 1] * near
        g, w = g[1 : n - 1], w[1 : n - 1]
    n = e.shape[0]
    wide = exact_dot(e.reshape(n * rows2, LANES), spread_table(LANES, LANES))
    wide = wide.reshape(n, rows2, LANES)
    spread2[:, pl.ds(0, rows2, 2), :] = wide
    spread2[:, pl.ds(1, rows2, 2), :] = wide
    origin = reach * half
    for q in range(-3, half + 3):
        a1[q + 3] = e1[origin + q] + spread2[(q + 4) // 2]

    def sweep1(source, start, stop, offset):
        e = source[start - offset : stop - offset]
        near = around(e, group1) + (
            source[start - 1 - offset : stop - 1 - offset]
            + source[start + 1 - offset : stop + 1 - offset]
        )
        window = slice(origin + start, origin + stop)
        return (1.0 - OMEGA) * e + scaled1[window] + weight1[window] * near

    for q in range(-2, half + 2, 4):
        b1[q + 2 : q + 6] = sweep1(a1, q, q + 4, -3)
    last = sweep1(b1, -1, half + 1, -2)
    n = last.shape[0]
    wide = exact_dot(last.reshape(n * rows1, LANES), spread_table(LANES, count * LANES))
    wide = wide.reshape(n, rows1, count * LANES)
    for i in range(count):
        part = wide[:, :, i * LANES : (i + 1) * LANES]
        spread1[i, :, pl.ds(0, rows1, 2), :] = part
        spread1[i, :, pl.ds(1, rows1, 2), :] = part
    for i in range(count):
        for p in range(depth + 4):
            a0[i, p] = estimate[i, p] + spread1[i, p // 2]
    for i in range(count):
        for p in range(depth + 2):
            e = a0[i, p + 1]
            near = around(e, LANES) + (a0[i, p] + a0[i, p + 2])
            b0[i, p] = (1.0 - OMEGA) * e + scaled[i, p] + weight[i, p] * near
    for i in range(count):
        for p in range(depth):
            e = b0[i, p + 1]
            near = around(e, LANES) + (b0[i, p] + b0[i, p + 2])
            update[i, p] = guess[i, p] + (
                (1.0 - OMEGA) * e + scaled[i, p + 1] + weight[i, p + 1] * near
            )


def row_sums(blocks, update, out, first):
    count, depth, rows = update.shape[:3]

    def body(x, totals):
        totals = list(totals)
        u = [update[i, x].reshape(rows // 8, 8, LANES) for i in range(count)]
        for r, block in enumerate(blocks):
            for j in range(count):
                o = block(j, x).reshape(rows // 8, 8, LANES)
                for i in range(count):
                    totals[(r * count + j) * count + i] += jnp.sum(o * u[i], axis=0)
        return tuple(totals)

    zero = jnp.zeros((8, LANES), F32)
    totals = lax.fori_loop(0, depth, body, (zero,) * (len(blocks) * count * count))
    for k, total in enumerate(totals):
        out[first + k : first + k + 1] = jnp.sum(total, axis=0, keepdims=True)


def reader(*refs):
    def read(j, x):
        value = refs[0][j, x]
        for ref in refs[1:]:
            value = value + ref[j, x]
        return value

    return read


def early_kernel(update, own, *refs):
    row_sums([reader(ref) for ref in (own,) + refs[:-1]], update, refs[-1], 0)


def late_kernel(update, early, *refs):
    last, out = refs[:-1], refs[-1]
    rows = early.shape[0]
    out[0:rows] = early[...]
    row_sums([reader(*last)], update, out, rows)


def project_kernel(blocks, parts, cells, update, own, *refs):
    others, last = refs[:blocks], refs[blocks : -3 - parts]
    sums, (out_ref, out, sems) = refs[-3 - parts : -3], refs[-3:]
    count, depth, _ = update.shape[:3]
    total = sums[0][...]
    for part in sums[1:]:
        total = total + part[...]
    overlap = jnp.sum(total, axis=1, keepdims=True) / cells
    reads = [reader(ref) for ref in (own,) + others] + [reader(*last)]

    def store(x):
        return pltpu.make_async_copy(out.at[:, x], out_ref.at[:, x], sems.at[x])

    for x in range(depth):
        values = [update[i, x] for i in range(count)]
        for r, read in enumerate(reads):
            for j in range(count):
                o = read(j, x)
                for i in range(count):
                    k = (r * count + j) * count + i
                    values[i] = values[i] - overlap[k : k + 1] * o
        for i in range(count):
            out[i, x] = values[i]
        store(x).start()
    for x in range(depth):
        store(x).wait()


def gather_blocks(block, axis):
    n = lax.axis_size(axis)
    if n == 4:
        first = lax.ppermute(block, axis, [(0, 2), (3, 1), (2, 3), (1, 0)])
        second = lax.ppermute(block, axis, [(1, 3), (2, 0), (0, 1), (3, 2)])
        inner = lax.ppermute(block, axis, [(1, 2), (2, 1)])
        outer = lax.ppermute(first, axis, [(2, 3), (1, 0)])
        return [first, second], [inner, outer]
    blocks = []
    for r in range(1, n):
        blocks.append(lax.ppermute(block, axis, [((i + r) % n, i) for i in range(n)]))
    return blocks[:-1], blocks[-1:]


def reduce_parts(value, axis):
    n = lax.axis_size(axis)
    if n & (n - 1):
        return [lax.psum(value, axis)]
    parts, stride, width = [value], 1, 2
    while stride < n:
        total = parts[0]
        for part in parts[1:]:
            total = total + part
        width = min(width, n // stride)
        parts = [total]
        for k in range(width - 1, 0, -1):
            pairs = [(i, i ^ (k * stride)) for i in range(n)]
            parts.append(lax.ppermute(total, axis, pairs))
        stride, width = stride * width, 4
    return parts


def on_device(orbitals, initial_guess, potential, perturbation, level_shifts, assignment):
    count, depth, ny, nz = orbitals.shape
    near = lambda x: pltpu.with_memory_space_constraint(x, pltpu.HBM)
    members = lax.axis_size("dom")
    half, rows1 = depth // 2, ny // 2
    assert nz == LANES and count * (nz // 2) == LANES and depth >= 2 * REACH
    plane = (ny, nz)
    shape = lambda *dims: jax.ShapeDtypeStruct(dims, F32)
    scratch = lambda *dims: pltpu.VMEM(dims, F32)
    params = pltpu.CompilerParams(vmem_limit_bytes=24 * 1024 * 1024)
    place = lax.axis_index("dom").astype(jnp.int32).reshape(1)

    blocks, last = gather_blocks(orbitals, "orb")

    message = (1 + REACH) * count + REACH
    inputs = tuple(
        map(near, (level_shifts, assignment, initial_guess, orbitals, potential, perturbation))
    )
    local = [
        pltpu.SMEM(level_shifts.shape, F32),
        pltpu.SMEM(assignment.shape, jnp.int32),
        scratch(count, depth, *plane),
        scratch(count, depth, *plane),
        scratch(depth, *plane),
        scratch(depth, *plane),
        pltpu.SemaphoreType.DMA((6,)),
    ]
    up, down = pl.pallas_call(
        edge_kernel,
        out_shape=(shape(message, *plane),) * 2,
        in_specs=[HBM] * 6,
        out_specs=(VMEM,) * 2,
        scratch_shapes=local,
        compiler_params=params,
    )(*inputs)
    own_scaled, own_weight = pl.pallas_call(
        own_kernel,
        out_shape=(shape(count, depth, *plane),) * 2,
        in_specs=[HBM] * 6,
        out_specs=(VMEM,) * 2,
        scratch_shapes=local,
        compiler_params=params,
    )(*inputs)
    low = lax.ppermute(up, "dom", [(i, (i + 1) % members) for i in range(members)])
    high = lax.ppermute(down, "dom", [((i + 1) % members, i) for i in range(members)])

    estimate, scaled, weight, payload = pl.pallas_call(
        fine_kernel,
        out_shape=(
            shape(count, depth + 4, *plane),
            shape(count, depth + 2, *plane),
            shape(count, depth + 2, *plane),
            shape(half + half // 2, rows1, LANES),
        ),
        in_specs=[SMEM, SMEM] + [VMEM] * 7,
        out_specs=(VMEM,) * 4,
        scratch_shapes=[
            scratch(count, depth + 2 * REACH, *plane),
            scratch(count, depth + 2 * REACH, *plane),
            scratch(half * count + half, *plane),
        ],
        compiler_params=params,
    )(level_shifts, assignment, near(own_scaled), near(own_weight), potential, low, high, up, down)

    gathered = lax.all_gather(payload, "dom", axis=0)

    window = 7 * half
    update = pl.pallas_call(
        coarse_kernel,
        out_shape=shape(count, depth, *plane),
        in_specs=[SMEM, SMEM, SMEM] + [VMEM] * 5,
        out_specs=VMEM,
        scratch_shapes=[
            scratch(window, rows1, LANES),
            scratch(window, rows1, LANES),
            scratch(window, rows1, LANES),
            scratch(window, rows1, LANES),
            scratch(2 * (window // 2 - 2), rows1, LANES),
            scratch(6, rows1, LANES),
            scratch(half + 6, rows1, LANES),
            scratch(half + 4, rows1, LANES),
            scratch(count, half + 2, *plane),
            scratch(count, depth + 4, *plane),
            scratch(count, depth + 2, *plane),
        ],
        compiler_params=params,
    )(place, level_shifts, assignment, gathered, estimate, scaled, weight, initial_guess)

    rows = (1 + len(blocks)) * count * count
    sums = pl.pallas_call(
        early_kernel,
        out_shape=shape(rows, LANES),
        in_specs=[VMEM] * (2 + len(blocks)),
        out_specs=VMEM,
        compiler_params=params,
    )(update, orbitals, *blocks)
    sums = pl.pallas_call(
        late_kernel,
        out_shape=shape(rows + count * count, LANES),
        in_specs=[VMEM] * (2 + len(last)),
        out_specs=VMEM,
        compiler_params=params,
    )(update, sums, *last)
    parts = reduce_parts(sums, "dom")
    cells = float(depth * members * ny * nz)
    return pl.pallas_call(
        functools.partial(project_kernel, len(blocks), len(parts), cells),
        out_shape=shape(count, depth, *plane),
        in_specs=[VMEM] * (2 + len(blocks) + len(last) + len(parts)),
        out_specs=HBM,
        scratch_shapes=[scratch(count, depth, *plane), pltpu.SemaphoreType.DMA((depth,))],
        compiler_params=params,
    )(update, orbitals, *blocks, *last, *parts)


def solution(mesh):
    in_specs = (
        P("orb", "dom", None, None),
        P("orb", "dom", None, None),
        P("dom", None, None),
        P("dom", None, None),
        P(),
        P("orb"),
    )
    return jax.shard_map(
        on_device,
        mesh=mesh,
        in_specs=in_specs,
        out_specs=P("orb", "dom", None, None),
        check_vma=False,
    )
```

```python
import functools

import jax
import jax.numpy as jnp
from jax import lax
from jax.experimental import pallas as pl
from jax.experimental.pallas import tpu as pltpu
from jax.sharding import PartitionSpec as P


OMEGA = 0.8
KINETIC = 8.0
LANES = 128
REACH = 3


F32 = jnp.float32
VMEM = pl.BlockSpec(memory_space=pltpu.VMEM)
SMEM = pl.BlockSpec(memory_space=pltpu.SMEM)
HBM = pl.BlockSpec(memory_space=pltpu.HBM)


def roll(x, shift, axis):
    return pltpu.roll(x, shift % x.shape[axis], axis)


def around(x, group):
    y, z = x.ndim - 2, x.ndim - 1
    total = roll(x, 1, y) + roll(x, -1, y)
    if group == x.shape[z]:
        return total + (roll(x, 1, z) + roll(x, -1, z))
    place = lax.broadcasted_iota(jnp.int32, x.shape, z) % group
    before = jnp.where(place == 0, roll(x, 1 - group, z), roll(x, 1, z))
    after = jnp.where(place == group - 1, roll(x, group - 1, z), roll(x, -1, z))
    return total + (before + after)


def exact_dot(values, table):
    high = values.astype(jnp.bfloat16)
    rest = values - high.astype(F32)
    middle = rest.astype(jnp.bfloat16)
    low = (rest - middle.astype(F32)).astype(jnp.bfloat16)
    dot = functools.partial(jnp.dot, preferred_element_type=F32)
    return dot(high, table) + (dot(middle, table) + dot(low, table))


def pair_table(rows, columns, value):
    r = lax.broadcasted_iota(jnp.int32, (rows, columns), 0)
    c = lax.broadcasted_iota(jnp.int32, (rows, columns), 1)
    return jnp.where(r // 2 == c, value, 0.0).astype(jnp.bfloat16)


def spread_table(rows, columns):
    r = lax.broadcasted_iota(jnp.int32, (rows, columns), 0)
    c = lax.broadcasted_iota(jnp.int32, (rows, columns), 1)
    return jnp.where(c // 2 == r, 1.0, 0.0).astype(jnp.bfloat16)


def load_all(pairs, sems):
    copies = [
        pltpu.make_async_copy(source, target, sems.at[k]) for k, (source, target) in enumerate(pairs)
    ]
    for copy in copies:
        copy.start()
    for copy in copies:
        copy.wait()


def own_source(i, x, constant, guess, orbital, potential, perturbation):
    value = guess[i, x]
    near = around(value, LANES)
    if x > 0:
        near = near + guess[i, x - 1]
    if x < guess.shape[1] - 1:
        near = near + guess[i, x + 1]
    return KINETIC * near - (constant + potential[x]) * value - perturbation[x] * orbital[i, x]


def edge_kernel(
    shifts_in, assigned_in, guess_in, orbital_in, potential_in, perturbation_in, up, down,
    shifts, assigned, guess, orbital, potential, perturbation, sems,
):
    fields = (guess, orbital, potential, perturbation)
    inputs = (shifts_in, assigned_in, guess_in, orbital_in, potential_in, perturbation_in)
    load_all(zip(inputs, (shifts, assigned) + fields), sems)
    count, depth = guess.shape[:2]
    for i in range(count):
        constant = 6.0 * KINETIC + shifts[assigned[i]]
        down[i] = guess[i, 0]
        up[i] = guess[i, depth - 1]
        for x in range(REACH):
            down[(1 + x) * count + i] = own_source(i, x, constant, *fields)
            up[(1 + x) * count + i] = own_source(i, depth - 1 - x, constant, *fields)
    for x in range(REACH):
        down[(1 + REACH) * count + x] = potential[x]
        up[(1 + REACH) * count + x] = potential[depth - 1 - x]


def own_kernel(
    shifts_in, assigned_in, guess_in, orbital_in, potential_in, perturbation_in, scaled, weight,
    shifts, assigned, guess, orbital, potential, perturbation, sems,
):
    fields = (guess, orbital, potential, perturbation)
    inputs = (shifts_in, assigned_in, guess_in, orbital_in, potential_in, perturbation_in)
    load_all(zip(inputs, (shifts, assigned) + fields), sems)
    count, depth = guess.shape[:2]
    for i in range(count):
        constant = 6.0 * KINETIC + shifts[assigned[i]]
        for x in range(depth):
            w = OMEGA / (constant + potential[x])
            weight[i, x] = KINETIC * w
            scaled[i, x] = w * own_source(i, x, constant, *fields)


def fine_kernel(
    shifts, assigned, own_scaled, own_weight, potential, low, high, up, down, estimate, scaled, weight, payload,
    all_scaled, all_weight, pairs,
):
    count, depth = own_scaled.shape[:2]
    planes = depth + 2 * REACH
    first = (1 + REACH) * count

    for i in range(count):
        constant = 6.0 * KINETIC + shifts[assigned[i]]
        for p in range(planes):
            x = p - REACH
            if 0 <= x < depth:
                kw = own_weight[i, x]
                g = own_scaled[i, x]
                if x == 0:
                    g = g + kw * low[i]
                if x == depth - 1:
                    g = g + kw * high[i]
            else:
                side, away = (low, -1 - x) if x < 0 else (high, x - depth)
                w = OMEGA / (constant + side[first + away])
                kw = KINETIC * w
                g = w * side[(1 + away) * count + i]
                if away == 0:
                    g = g + kw * (down if x < 0 else up)[i]
            all_weight[i, p] = kw
            all_scaled[i, p] = g
            if 2 <= p < planes - 2:
                scaled[i, p - 2] = g
                weight[i, p - 2] = kw
    for i in range(count):
        for p in range(1, planes - 1):
            g = all_scaled[i, p]
            near = around(g, LANES) + (all_scaled[i, p - 1] + all_scaled[i, p + 1])
            estimate[i, p - 1] = (2.0 - OMEGA) * g + all_weight[i, p] * near
    half = depth // 2
    for i in range(count):
        constant = 6.0 * KINETIC + shifts[assigned[i]]
        for q in range(half):
            total = None
            for x in (2 * q, 2 * q + 1):
                e = estimate[i, x + 2]
                near = around(e, LANES) + (estimate[i, x + 1] + estimate[i, x + 3])
                r = (constant + potential[x]) * (
                    (1.0 / OMEGA) * all_scaled[i, x + REACH] - e
                ) + KINETIC * near
                total = r if total is None else total + r
            pairs[q * count + i] = total
    for q in range(half):
        pairs[half * count + q] = potential[2 * q] + potential[2 * q + 1]
    rows = pairs.shape[1] // 2
    slots = pairs.shape[0] // 2
    even = pairs[:, pl.ds(0, rows, 2), :] + pairs[:, pl.ds(1, rows, 2), :]
    even = even.reshape(slots, 2, rows, LANES)
    both = jnp.concatenate([even[:, 0], even[:, 1]], axis=-1).reshape(slots * rows, 2 * LANES)
    payload[...] = exact_dot(both, pair_table(2 * LANES, LANES, 0.125)).reshape(slots, rows, LANES)


def coarse_kernel(
    place, shifts, assigned, gathered, estimate, scaled, weight, guess, update,
    scaled1, weight1, coef1, e1, pairs, spread2, a1, b1, spread1, a0, b0,
):
    members = gathered.shape[0]
    count, depth = guess.shape[:2]
    half = depth // 2
    reach = 3
    window = (2 * reach + 1) * half
    rows1 = gathered.shape[2]
    group1 = LANES // count
    k1 = KINETIC / 4
    k2 = KINETIC / 16

    def shift_lanes(group):
        lane = lax.broadcasted_iota(jnp.int32, (1, 1, LANES), 2) // group
        value = jnp.full((1, 1, LANES), shifts[assigned[0]], F32)
        for i in range(1, count):
            value = jnp.where(lane % count == i, shifts[assigned[i]], value)
        return value

    base1 = 6.0 * k1 + shift_lanes(group1)
    base2 = 6.0 * k2 + shift_lanes(group1 // 2)
    lane = lax.broadcasted_iota(jnp.int32, (1, rows1, LANES), 2)
    for s in range(2 * reach + 1):
        slot = lax.rem(place[0] + (s - reach + 2 * members), members)
        f = gathered[slot, 0:half]
        for t in range(half // 2):
            packed = gathered[slot, half + t : half + t + 1]
            swapped = roll(packed, LANES // 2, 2)
            coef1[s * half + 2 * t : s * half + 2 * t + 1] = jnp.where(
                lane < LANES // 2, packed, swapped
            )
            coef1[s * half + 2 * t + 1 : s * half + 2 * t + 2] = jnp.where(
                lane < LANES // 2, swapped, packed
            )
        w = OMEGA / (base1 + coef1[s * half : (s + 1) * half])
        weight1[s * half : (s + 1) * half] = k1 * w
        scaled1[s * half : (s + 1) * half] = w * f
    step = 4
    for p in range(1, window - 1, step):
        stop = min(p + step, window - 1)
        g = scaled1[p:stop]
        near = around(g, group1) + (scaled1[p - 1 : stop - 1] + scaled1[p + 1 : stop + 1])
        e1[p:stop] = (2.0 - OMEGA) * g + weight1[p:stop] * near
    coarse = window // 2 - 2
    for p in range(2, window - 2, step):
        stop = min(p + step, window - 2)
        e = e1[p:stop]
        near = around(e, group1) + (e1[p - 1 : stop - 1] + e1[p + 1 : stop + 1])
        c = coef1[p:stop]
        r = (base1 + c) * ((1.0 / OMEGA) * scaled1[p:stop] - e) + k1 * near
        for t in range(0, stop - p, 2):
            pairs[(p + t) // 2 - 1] = r[t] + r[t + 1]
            pairs[coarse + (p + t) // 2 - 1] = c[t] + c[t + 1]
    rows2 = rows1 // 2
    even = pairs[:, pl.ds(0, rows2, 2), :] + pairs[:, pl.ds(1, rows2, 2), :]
    both = exact_dot(
        even.reshape(2 * coarse * rows2, LANES), pair_table(LANES, LANES, 0.125)
    ).reshape(2 * coarse, rows2, LANES)
    w = OMEGA / (base2 + both[coarse:])
    g = w * both[:coarse]
    w = k2 * w
    e = None
    for _ in range(3):
        n = g.shape[0]
        if e is None:
            e = g
            mine = (2.0 - OMEGA) * g[1 : n - 1]
        else:
            mine = (1.0 - OMEGA) * e[1 : n - 1] + g[1 : n - 1]
        near = around(e[1 : n - 1], group1 // 2) + (e[0 : n - 2] + e[2:n])
        e = mine + w[1 : n - 1] * near
        g, w = g[1 : n - 1], w[1 : n - 1]
    n = e.shape[0]
    wide = exact_dot(e.reshape(n * rows2, LANES), spread_table(LANES, LANES))
    wide = wide.reshape(n, rows2, LANES)
    spread2[:, pl.ds(0, rows2, 2), :] = wide
    spread2[:, pl.ds(1, rows2, 2), :] = wide
    origin = reach * half
    for q in range(-3, half + 3):
        a1[q + 3] = e1[origin + q] + spread2[(q + 4) // 2]

    def sweep1(source, start, stop, offset):
        e = source[start - offset : stop - offset]
        near = around(e, group1) + (
            source[start - 1 - offset : stop - 1 - offset]
            + source[start + 1 - offset : stop + 1 - offset]
        )
        window = slice(origin + start, origin + stop)
        return (1.0 - OMEGA) * e + scaled1[window] + weight1[window] * near

    for q in range(-2, half + 2, 4):
        b1[q + 2 : q + 6] = sweep1(a1, q, q + 4, -3)
    last = sweep1(b1, -1, half + 1, -2)
    n = last.shape[0]
    wide = exact_dot(last.reshape(n * rows1, LANES), spread_table(LANES, count * LANES))
    wide = wide.reshape(n, rows1, count * LANES)
    for i in range(count):
        part = wide[:, :, i * LANES : (i + 1) * LANES]
        spread1[i, :, pl.ds(0, rows1, 2), :] = part
        spread1[i, :, pl.ds(1, rows1, 2), :] = part
    for i in range(count):
        for p in range(depth + 4):
            a0[i, p] = estimate[i, p] + spread1[i, p // 2]
    for i in range(count):
        for p in range(depth + 2):
            e = a0[i, p + 1]
            near = around(e, LANES) + (a0[i, p] + a0[i, p + 2])
            b0[i, p] = (1.0 - OMEGA) * e + scaled[i, p] + weight[i, p] * near
    for i in range(count):
        for p in range(depth):
            e = b0[i, p + 1]
            near = around(e, LANES) + (b0[i, p] + b0[i, p + 2])
            update[i, p] = guess[i, p] + (
                (1.0 - OMEGA) * e + scaled[i, p + 1] + weight[i, p + 1] * near
            )


def row_sums(blocks, update, out, first):
    count, depth, rows = update.shape[:3]

    def body(x, totals):
        totals = list(totals)
        u = [update[i, x].reshape(rows // 8, 8, LANES) for i in range(count)]
        for r, block in enumerate(blocks):
            for j in range(count):
                o = block(j, x).reshape(rows // 8, 8, LANES)
                for i in range(count):
                    totals[(r * count + j) * count + i] += jnp.sum(o * u[i], axis=0)
        return tuple(totals)

    zero = jnp.zeros((8, LANES), F32)
    totals = lax.fori_loop(0, depth, body, (zero,) * (len(blocks) * count * count))
    for k, total in enumerate(totals):
        out[first + k : first + k + 1] = jnp.sum(total, axis=0, keepdims=True)


def reader(ref, other=None, use_other=None):
    def read(j, x):
        if other is None:
            return ref[j, x]
        return jnp.where(use_other, other[j, x], ref[j, x])

    return read


def chosen(last, outside):
    return (outside[0] == 1,) if len(last) == 2 else ()


def early_kernel(update, own, *refs):
    row_sums([reader(ref) for ref in (own,) + refs[:-1]], update, refs[-1], 0)


def late_kernel(outside, update, early, *refs):
    last, out = refs[:-1], refs[-1]
    rows = early.shape[0]
    out[0:rows] = early[...]
    row_sums([reader(*last, *chosen(last, outside))], update, out, rows)


def project_kernel(blocks, parts, cells, outside, update, own, *refs):
    others, last = refs[:blocks], refs[blocks : -3 - parts]
    sums, (out_ref, out, sems) = refs[-3 - parts : -3], refs[-3:]
    count, depth, _ = update.shape[:3]
    total = sums[0][...]
    for part in sums[1:]:
        total = total + part[...]
    overlap = jnp.sum(total, axis=1, keepdims=True) / cells
    reads = [reader(ref) for ref in (own,) + others] + [reader(*last, *chosen(last, outside))]

    def store(x):
        return pltpu.make_async_copy(out.at[:, x], out_ref.at[:, x], sems.at[x])

    for x in range(depth):
        values = [update[i, x] for i in range(count)]
        for r, read in enumerate(reads):
            for j in range(count):
                o = read(j, x)
                for i in range(count):
                    k = (r * count + j) * count + i
                    values[i] = values[i] - overlap[k : k + 1] * o
        for i in range(count):
            out[i, x] = values[i]
        store(x).start()
    for x in range(depth):
        store(x).wait()


def gather_blocks(block, axis):
    n = lax.axis_size(axis)
    if n == 4:
        first = lax.ppermute(block, axis, [(0, 2), (3, 1), (2, 3), (1, 0)])
        second = lax.ppermute(block, axis, [(1, 3), (2, 0), (0, 1), (3, 2)])
        inner = lax.ppermute(block, axis, [(1, 2), (2, 1), (0, 0), (3, 3)])
        outer = lax.ppermute(first, axis, [(2, 3), (1, 0), (0, 1), (3, 2)])
        return [first, second], [inner, outer]
    blocks = []
    for r in range(1, n):
        blocks.append(lax.ppermute(block, axis, [((i + r) % n, i) for i in range(n)]))
    return blocks[:-1], blocks[-1:]


def reduce_parts(value, axis):
    n = lax.axis_size(axis)
    if n & (n - 1):
        return [lax.psum(value, axis)]
    parts, stride, width = [value], 1, 2
    while stride < n:
        total = parts[0]
        for part in parts[1:]:
            total = total + part
        width = min(width, n // stride)
        parts = [total]
        for k in range(width - 1, 0, -1):
            pairs = [(i, i ^ (k * stride)) for i in range(n)]
            parts.append(lax.ppermute(total, axis, pairs))
        stride, width = stride * width, 4
    return parts


def on_device(orbitals, initial_guess, potential, perturbation, level_shifts, assignment):
    count, depth, ny, nz = orbitals.shape
    near = lambda x: pltpu.with_memory_space_constraint(x, pltpu.HBM)
    members = lax.axis_size("dom")
    half, rows1 = depth // 2, ny // 2
    assert nz == LANES and count * (nz // 2) == LANES and depth >= 2 * REACH
    plane = (ny, nz)
    shape = lambda *dims: jax.ShapeDtypeStruct(dims, F32)
    scratch = lambda *dims: pltpu.VMEM(dims, F32)
    params = pltpu.CompilerParams(vmem_limit_bytes=24 * 1024 * 1024)
    place = lax.axis_index("dom").astype(jnp.int32).reshape(1)

    blocks, last = gather_blocks(orbitals, "orb")
    rank = lax.axis_index("orb")
    outside = jnp.logical_or(rank == 0, rank == lax.axis_size("orb") - 1).astype(jnp.int32).reshape(1)

    message = (1 + REACH) * count + REACH
    inputs = tuple(
        map(near, (level_shifts, assignment, initial_guess, orbitals, potential, perturbation))
    )
    local = [
        pltpu.SMEM(level_shifts.shape, F32),
        pltpu.SMEM(assignment.shape, jnp.int32),
        scratch(count, depth, *plane),
        scratch(count, depth, *plane),
        scratch(depth, *plane),
        scratch(depth, *plane),
        pltpu.SemaphoreType.DMA((6,)),
    ]
    up, down = pl.pallas_call(
        edge_kernel,
        out_shape=(shape(message, *plane),) * 2,
        in_specs=[HBM] * 6,
        out_specs=(VMEM,) * 2,
        scratch_shapes=local,
        compiler_params=params,
    )(*inputs)
    own_scaled, own_weight = pl.pallas_call(
        own_kernel,
        out_shape=(shape(count, depth, *plane),) * 2,
        in_specs=[HBM] * 6,
        out_specs=(VMEM,) * 2,
        scratch_shapes=local,
        compiler_params=params,
    )(*inputs)
    low = lax.ppermute(up, "dom", [(i, (i + 1) % members) for i in range(members)])
    high = lax.ppermute(down, "dom", [((i + 1) % members, i) for i in range(members)])

    estimate, scaled, weight, payload = pl.pallas_call(
        fine_kernel,
        out_shape=(
            shape(count, depth + 4, *plane),
            shape(count, depth + 2, *plane),
            shape(count, depth + 2, *plane),
            shape(half + half // 2, rows1, LANES),
        ),
        in_specs=[SMEM, SMEM] + [VMEM] * 7,
        out_specs=(VMEM,) * 4,
        scratch_shapes=[
            scratch(count, depth + 2 * REACH, *plane),
            scratch(count, depth + 2 * REACH, *plane),
            scratch(half * count + half, *plane),
        ],
        compiler_params=params,
    )(level_shifts, assignment, near(own_scaled), near(own_weight), potential, low, high, up, down)

    gathered = lax.all_gather(payload, "dom", axis=0)

    window = 7 * half
    update = pl.pallas_call(
        coarse_kernel,
        out_shape=shape(count, depth, *plane),
        in_specs=[SMEM, SMEM, SMEM] + [VMEM] * 5,
        out_specs=VMEM,
        scratch_shapes=[
            scratch(window, rows1, LANES),
            scratch(window, rows1, LANES),
            scratch(window, rows1, LANES),
            scratch(window, rows1, LANES),
            scratch(2 * (window // 2 - 2), rows1, LANES),
            scratch(6, rows1, LANES),
            scratch(half + 6, rows1, LANES),
            scratch(half + 4, rows1, LANES),
            scratch(count, half + 2, *plane),
            scratch(count, depth + 4, *plane),
            scratch(count, depth + 2, *plane),
        ],
        compiler_params=params,
    )(place, level_shifts, assignment, gathered, estimate, scaled, weight, initial_guess)

    rows = (1 + len(blocks)) * count * count
    sums = pl.pallas_call(
        early_kernel,
        out_shape=shape(rows, LANES),
        in_specs=[VMEM] * (2 + len(blocks)),
        out_specs=VMEM,
        compiler_params=params,
    )(update, orbitals, *blocks)
    sums = pl.pallas_call(
        late_kernel,
        out_shape=shape(rows + count * count, LANES),
        in_specs=[SMEM] + [VMEM] * (2 + len(last)),
        out_specs=VMEM,
        compiler_params=params,
    )(outside, update, sums, *last)
    parts = reduce_parts(sums, "dom")
    cells = float(depth * members * ny * nz)
    return pl.pallas_call(
        functools.partial(project_kernel, len(blocks), len(parts), cells),
        out_shape=shape(count, depth, *plane),
        in_specs=[SMEM] + [VMEM] * (2 + len(blocks) + len(last) + len(parts)),
        out_specs=HBM,
        scratch_shapes=[scratch(count, depth, *plane), pltpu.SemaphoreType.DMA((depth,))],
        compiler_params=params,
    )(outside, update, orbitals, *blocks, *last, *parts)


def solution(mesh):
    in_specs = (
        P("orb", "dom", None, None),
        P("orb", "dom", None, None),
        P("dom", None, None),
        P("dom", None, None),
        P(),
        P("orb"),
    )
    return jax.shard_map(
        on_device,
        mesh=mesh,
        in_specs=in_specs,
        out_specs=P("orb", "dom", None, None),
        check_vma=False,
    )
```

```python
import functools

import jax
import jax.numpy as jnp
from jax import lax
from jax.experimental import pallas as pl
from jax.experimental.pallas import tpu as pltpu
from jax.sharding import PartitionSpec as P


OMEGA = 0.8
KINETIC = 8.0
LANES = 128
REACH = 3


F32 = jnp.float32
VMEM = pl.BlockSpec(memory_space=pltpu.VMEM)
SMEM = pl.BlockSpec(memory_space=pltpu.SMEM)
HBM = pl.BlockSpec(memory_space=pltpu.HBM)


def roll(x, shift, axis):
    return pltpu.roll(x, shift % x.shape[axis], axis)


def around(x, group):
    y, z = x.ndim - 2, x.ndim - 1
    total = roll(x, 1, y) + roll(x, -1, y)
    if group == x.shape[z]:
        return total + (roll(x, 1, z) + roll(x, -1, z))
    place = lax.broadcasted_iota(jnp.int32, x.shape, z) % group
    before = jnp.where(place == 0, roll(x, 1 - group, z), roll(x, 1, z))
    after = jnp.where(place == group - 1, roll(x, group - 1, z), roll(x, -1, z))
    return total + (before + after)


def exact_dot(values, table):
    high = values.astype(jnp.bfloat16)
    rest = values - high.astype(F32)
    middle = rest.astype(jnp.bfloat16)
    low = (rest - middle.astype(F32)).astype(jnp.bfloat16)
    dot = functools.partial(jnp.dot, preferred_element_type=F32)
    return dot(high, table) + (dot(middle, table) + dot(low, table))


def pair_table(rows, columns, value):
    r = lax.broadcasted_iota(jnp.int32, (rows, columns), 0)
    c = lax.broadcasted_iota(jnp.int32, (rows, columns), 1)
    return jnp.where(r // 2 == c, value, 0.0).astype(jnp.bfloat16)


def spread_table(rows, columns):
    r = lax.broadcasted_iota(jnp.int32, (rows, columns), 0)
    c = lax.broadcasted_iota(jnp.int32, (rows, columns), 1)
    return jnp.where(c // 2 == r, 1.0, 0.0).astype(jnp.bfloat16)


def load_all(pairs, sems):
    copies = [
        pltpu.make_async_copy(source, target, sems.at[k]) for k, (source, target) in enumerate(pairs)
    ]
    for copy in copies:
        copy.start()
    for copy in copies:
        copy.wait()


def own_source(i, x, constant, guess, orbital, potential, perturbation):
    value = guess[i, x]
    near = around(value, LANES)
    if x > 0:
        near = near + guess[i, x - 1]
    if x < guess.shape[1] - 1:
        near = near + guess[i, x + 1]
    return KINETIC * near - (constant + potential[x]) * value - perturbation[x] * orbital[i, x]


def edge_kernel(
    shifts_in, assigned_in, guess_in, orbital_in, potential_in, perturbation_in, up, down,
    shifts, assigned, guess, orbital, potential, perturbation, sems,
):
    fields = (guess, orbital, potential, perturbation)
    inputs = (shifts_in, assigned_in, guess_in, orbital_in, potential_in, perturbation_in)
    load_all(zip(inputs, (shifts, assigned) + fields), sems)
    count, depth = guess.shape[:2]
    for i in range(count):
        constant = 6.0 * KINETIC + shifts[assigned[i]]
        down[i] = guess[i, 0]
        up[i] = guess[i, depth - 1]
        for x in range(REACH):
            down[(1 + x) * count + i] = own_source(i, x, constant, *fields)
            up[(1 + x) * count + i] = own_source(i, depth - 1 - x, constant, *fields)
    for x in range(REACH):
        down[(1 + REACH) * count + x] = potential[x]
        up[(1 + REACH) * count + x] = potential[depth - 1 - x]


def own_kernel(
    shifts_in, assigned_in, guess_in, orbital_in, potential_in, perturbation_in, scaled, weight,
    shifts, assigned, guess, orbital, potential, perturbation, sems,
):
    fields = (guess, orbital, potential, perturbation)
    inputs = (shifts_in, assigned_in, guess_in, orbital_in, potential_in, perturbation_in)
    load_all(zip(inputs, (shifts, assigned) + fields), sems)
    count, depth = guess.shape[:2]
    for i in range(count):
        constant = 6.0 * KINETIC + shifts[assigned[i]]
        for x in range(depth):
            w = OMEGA / (constant + potential[x])
            weight[i, x] = KINETIC * w
            scaled[i, x] = w * own_source(i, x, constant, *fields)


def fine_kernel(
    shifts, assigned, own_scaled, own_weight, potential, low, high, up, down, estimate, scaled, weight, payload,
    all_scaled, all_weight, pairs,
):
    count, depth = own_scaled.shape[:2]
    planes = depth + 2 * REACH
    first = (1 + REACH) * count

    for i in range(count):
        constant = 6.0 * KINETIC + shifts[assigned[i]]
        for p in range(planes):
            x = p - REACH
            if 0 <= x < depth:
                kw = own_weight[i, x]
                g = own_scaled[i, x]
                if x == 0:
                    g = g + kw * low[i]
                if x == depth - 1:
                    g = g + kw * high[i]
            else:
                side, away = (low, -1 - x) if x < 0 else (high, x - depth)
                w = OMEGA / (constant + side[first + away])
                kw = KINETIC * w
                g = w * side[(1 + away) * count + i]
                if away == 0:
                    g = g + kw * (down if x < 0 else up)[i]
            all_weight[i, p] = kw
            all_scaled[i, p] = g
            if 2 <= p < planes - 2:
                scaled[i, p - 2] = g
                weight[i, p - 2] = kw
    for i in range(count):
        for p in range(1, planes - 1):
            g = all_scaled[i, p]
            near = around(g, LANES) + (all_scaled[i, p - 1] + all_scaled[i, p + 1])
            estimate[i, p - 1] = (2.0 - OMEGA) * g + all_weight[i, p] * near
    half = depth // 2
    for i in range(count):
        constant = 6.0 * KINETIC + shifts[assigned[i]]
        for q in range(half):
            total = None
            for x in (2 * q, 2 * q + 1):
                e = estimate[i, x + 2]
                near = around(e, LANES) + (estimate[i, x + 1] + estimate[i, x + 3])
                r = (constant + potential[x]) * (
                    (1.0 / OMEGA) * all_scaled[i, x + REACH] - e
                ) + KINETIC * near
                total = r if total is None else total + r
            pairs[q * count + i] = total
    for q in range(half):
        pairs[half * count + q] = potential[2 * q] + potential[2 * q + 1]
    rows = pairs.shape[1] // 2
    slots = pairs.shape[0] // 2
    even = pairs[:, pl.ds(0, rows, 2), :] + pairs[:, pl.ds(1, rows, 2), :]
    even = even.reshape(slots, 2, rows, LANES)
    both = jnp.concatenate([even[:, 0], even[:, 1]], axis=-1).reshape(slots * rows, 2 * LANES)
    payload[...] = exact_dot(both, pair_table(2 * LANES, LANES, 0.125)).reshape(slots, rows, LANES)


def coarse_kernel(
    place, shifts, assigned, gathered, estimate, scaled, weight, guess, update,
    scaled1, weight1, coef1, e1, pairs, spread2, a1, b1, spread1, a0, b0,
):
    members = gathered.shape[0]
    count, depth = guess.shape[:2]
    half = depth // 2
    reach = 3
    window = (2 * reach + 1) * half
    rows1 = gathered.shape[2]
    group1 = LANES // count
    k1 = KINETIC / 4
    k2 = KINETIC / 16

    def shift_lanes(group):
        lane = lax.broadcasted_iota(jnp.int32, (1, 1, LANES), 2) // group
        value = jnp.full((1, 1, LANES), shifts[assigned[0]], F32)
        for i in range(1, count):
            value = jnp.where(lane % count == i, shifts[assigned[i]], value)
        return value

    base1 = 6.0 * k1 + shift_lanes(group1)
    base2 = 6.0 * k2 + shift_lanes(group1 // 2)
    lane = lax.broadcasted_iota(jnp.int32, (1, rows1, LANES), 2)
    for s in range(2 * reach + 1):
        slot = lax.rem(place[0] + (s - reach + 2 * members), members)
        f = gathered[slot, 0:half]
        for t in range(half // 2):
            packed = gathered[slot, half + t : half + t + 1]
            swapped = roll(packed, LANES // 2, 2)
            coef1[s * half + 2 * t : s * half + 2 * t + 1] = jnp.where(
                lane < LANES // 2, packed, swapped
            )
            coef1[s * half + 2 * t + 1 : s * half + 2 * t + 2] = jnp.where(
                lane < LANES // 2, swapped, packed
            )
        w = OMEGA / (base1 + coef1[s * half : (s + 1) * half])
        weight1[s * half : (s + 1) * half] = k1 * w
        scaled1[s * half : (s + 1) * half] = w * f
    step = 4
    for p in range(1, window - 1, step):
        stop = min(p + step, window - 1)
        g = scaled1[p:stop]
        near = around(g, group1) + (scaled1[p - 1 : stop - 1] + scaled1[p + 1 : stop + 1])
        e1[p:stop] = (2.0 - OMEGA) * g + weight1[p:stop] * near
    coarse = window // 2 - 2
    for p in range(2, window - 2, step):
        stop = min(p + step, window - 2)
        e = e1[p:stop]
        near = around(e, group1) + (e1[p - 1 : stop - 1] + e1[p + 1 : stop + 1])
        c = coef1[p:stop]
        r = (base1 + c) * ((1.0 / OMEGA) * scaled1[p:stop] - e) + k1 * near
        for t in range(0, stop - p, 2):
            pairs[(p + t) // 2 - 1] = r[t] + r[t + 1]
            pairs[coarse + (p + t) // 2 - 1] = c[t] + c[t + 1]
    rows2 = rows1 // 2
    even = pairs[:, pl.ds(0, rows2, 2), :] + pairs[:, pl.ds(1, rows2, 2), :]
    both = exact_dot(
        even.reshape(2 * coarse * rows2, LANES), pair_table(LANES, LANES, 0.125)
    ).reshape(2 * coarse, rows2, LANES)
    w = OMEGA / (base2 + both[coarse:])
    g = w * both[:coarse]
    w = k2 * w
    e = None
    for _ in range(3):
        n = g.shape[0]
        if e is None:
            e = g
            mine = (2.0 - OMEGA) * g[1 : n - 1]
        else:
            mine = (1.0 - OMEGA) * e[1 : n - 1] + g[1 : n - 1]
        near = around(e[1 : n - 1], group1 // 2) + (e[0 : n - 2] + e[2:n])
        e = mine + w[1 : n - 1] * near
        g, w = g[1 : n - 1], w[1 : n - 1]
    n = e.shape[0]
    wide = exact_dot(e.reshape(n * rows2, LANES), spread_table(LANES, LANES))
    wide = wide.reshape(n, rows2, LANES)
    spread2[:, pl.ds(0, rows2, 2), :] = wide
    spread2[:, pl.ds(1, rows2, 2), :] = wide
    origin = reach * half
    for q in range(-3, half + 3):
        a1[q + 3] = e1[origin + q] + spread2[(q + 4) // 2]

    def sweep1(source, start, stop, offset):
        e = source[start - offset : stop - offset]
        near = around(e, group1) + (
            source[start - 1 - offset : stop - 1 - offset]
            + source[start + 1 - offset : stop + 1 - offset]
        )
        window = slice(origin + start, origin + stop)
        return (1.0 - OMEGA) * e + scaled1[window] + weight1[window] * near

    for q in range(-2, half + 2, 4):
        b1[q + 2 : q + 6] = sweep1(a1, q, q + 4, -3)
    last = sweep1(b1, -1, half + 1, -2)
    n = last.shape[0]
    wide = exact_dot(last.reshape(n * rows1, LANES), spread_table(LANES, count * LANES))
    wide = wide.reshape(n, rows1, count * LANES)
    for i in range(count):
        part = wide[:, :, i * LANES : (i + 1) * LANES]
        spread1[i, :, pl.ds(0, rows1, 2), :] = part
        spread1[i, :, pl.ds(1, rows1, 2), :] = part
    for i in range(count):
        for p in range(depth + 4):
            a0[i, p] = estimate[i, p] + spread1[i, p // 2]
    for i in range(count):
        for p in range(depth + 2):
            e = a0[i, p + 1]
            near = around(e, LANES) + (a0[i, p] + a0[i, p + 2])
            b0[i, p] = (1.0 - OMEGA) * e + scaled[i, p] + weight[i, p] * near
    for i in range(count):
        for p in range(depth):
            e = b0[i, p + 1]
            near = around(e, LANES) + (b0[i, p] + b0[i, p + 2])
            update[i, p] = guess[i, p] + (
                (1.0 - OMEGA) * e + scaled[i, p + 1] + weight[i, p + 1] * near
            )


def row_sums(blocks, update, out, first):
    count, depth, rows = update.shape[:3]

    def body(x, totals):
        totals = list(totals)
        u = [update[i, x].reshape(rows // 8, 8, LANES) for i in range(count)]
        for r, block in enumerate(blocks):
            for j in range(count):
                o = block(j, x).reshape(rows // 8, 8, LANES)
                for i in range(count):
                    totals[(r * count + j) * count + i] += jnp.sum(o * u[i], axis=0)
        return tuple(totals)

    zero = jnp.zeros((8, LANES), F32)
    totals = lax.fori_loop(0, depth, body, (zero,) * (len(blocks) * count * count))
    for k, total in enumerate(totals):
        out[first + k : first + k + 1] = jnp.sum(total, axis=0, keepdims=True)


def reader(ref, other=None, use_other=None):
    def read(j, x):
        if other is None:
            return ref[j, x]
        return jnp.where(use_other, other[j, x], ref[j, x])

    return read


def chosen(last, outside):
    return (outside[0] == 1,) if len(last) == 2 else ()


def early_kernel(update, own, *refs):
    row_sums([reader(ref) for ref in (own,) + refs[:-1]], update, refs[-1], 0)


def lane_of(rows):
    place = (rows, LANES)
    return lax.broadcasted_iota(jnp.int32, place, 0) == lax.broadcasted_iota(jnp.int32, place, 1)


def late_kernel(outside, update, early, *refs):
    last, (out, sums) = refs[:-2], refs[-2:]
    rows = early.shape[0]
    sums[0:rows] = early[...]
    row_sums([reader(*last, *chosen(last, outside))], update, sums, rows)
    total = jnp.sum(sums[...], axis=1, keepdims=True)
    out[...] = jnp.sum(jnp.where(lane_of(sums.shape[0]), total, 0.0), axis=0, keepdims=True)


def project_kernel(blocks, parts, cells, outside, update, own, *refs):
    others, last = refs[:blocks], refs[blocks : -3 - parts]
    sums, (out_ref, out, sems) = refs[-3 - parts : -3], refs[-3:]
    count, depth, _ = update.shape[:3]
    total = sums[0][...]
    for part in sums[1:]:
        total = total + part[...]
    pairs = (2 + blocks) * count * count
    spread = jnp.where(lane_of(pairs), jnp.broadcast_to(total, (pairs, LANES)), 0.0)
    overlap = jnp.sum(spread, axis=1, keepdims=True) / cells
    reads = [reader(ref) for ref in (own,) + others] + [reader(*last, *chosen(last, outside))]

    def store(x):
        return pltpu.make_async_copy(out.at[:, x], out_ref.at[:, x], sems.at[x])

    for x in range(depth):
        values = [update[i, x] for i in range(count)]
        for r, read in enumerate(reads):
            for j in range(count):
                o = read(j, x)
                for i in range(count):
                    k = (r * count + j) * count + i
                    values[i] = values[i] - overlap[k : k + 1] * o
        for i in range(count):
            out[i, x] = values[i]
        store(x).start()
    for x in range(depth):
        store(x).wait()


def gather_blocks(block, axis):
    n = lax.axis_size(axis)
    if n == 4:
        first = lax.ppermute(block, axis, [(0, 2), (3, 1), (2, 3), (1, 0)])
        second = lax.ppermute(block, axis, [(1, 3), (2, 0), (0, 1), (3, 2)])
        inner = lax.ppermute(block, axis, [(1, 2), (2, 1), (0, 0), (3, 3)])
        outer = lax.ppermute(first, axis, [(2, 3), (1, 0), (0, 1), (3, 2)])
        return [first, second], [inner, outer]
    blocks = []
    for r in range(1, n):
        blocks.append(lax.ppermute(block, axis, [((i + r) % n, i) for i in range(n)]))
    return blocks[:-1], blocks[-1:]


def reduce_parts(value, axis):
    n = lax.axis_size(axis)
    if n & (n - 1):
        return [lax.psum(value, axis)]
    parts, top = [value], n
    while top > 1:
        total = parts[0]
        for part in parts[1:]:
            total = total + part
        width = min(4, top // 2) if top > 2 else 2
        top //= width
        parts = [total]
        for k in range(width - 1, 0, -1):
            pairs = [(i, i ^ (k * top)) for i in range(n)]
            parts.append(lax.ppermute(total, axis, pairs))
    return parts


def on_device(orbitals, initial_guess, potential, perturbation, level_shifts, assignment):
    count, depth, ny, nz = orbitals.shape
    near = lambda x: pltpu.with_memory_space_constraint(x, pltpu.HBM)
    members = lax.axis_size("dom")
    half, rows1 = depth // 2, ny // 2
    assert nz == LANES and count * (nz // 2) == LANES and depth >= 2 * REACH
    plane = (ny, nz)
    shape = lambda *dims: jax.ShapeDtypeStruct(dims, F32)
    scratch = lambda *dims: pltpu.VMEM(dims, F32)
    params = pltpu.CompilerParams(vmem_limit_bytes=24 * 1024 * 1024)
    place = lax.axis_index("dom").astype(jnp.int32).reshape(1)

    blocks, last = gather_blocks(orbitals, "orb")
    rank = lax.axis_index("orb")
    outside = jnp.logical_or(rank == 0, rank == lax.axis_size("orb") - 1).astype(jnp.int32).reshape(1)

    message = (1 + REACH) * count + REACH
    inputs = tuple(
        map(near, (level_shifts, assignment, initial_guess, orbitals, potential, perturbation))
    )
    local = [
        pltpu.SMEM(level_shifts.shape, F32),
        pltpu.SMEM(assignment.shape, jnp.int32),
        scratch(count, depth, *plane),
        scratch(count, depth, *plane),
        scratch(depth, *plane),
        scratch(depth, *plane),
        pltpu.SemaphoreType.DMA((6,)),
    ]
    up, down = pl.pallas_call(
        edge_kernel,
        out_shape=(shape(message, *plane),) * 2,
        in_specs=[HBM] * 6,
        out_specs=(VMEM,) * 2,
        scratch_shapes=local,
        compiler_params=params,
    )(*inputs)
    own_scaled, own_weight = pl.pallas_call(
        own_kernel,
        out_shape=(shape(count, depth, *plane),) * 2,
        in_specs=[HBM] * 6,
        out_specs=(VMEM,) * 2,
        scratch_shapes=local,
        compiler_params=params,
    )(*inputs)
    low = lax.ppermute(up, "dom", [(i, (i + 1) % members) for i in range(members)])
    high = lax.ppermute(down, "dom", [((i + 1) % members, i) for i in range(members)])

    estimate, scaled, weight, payload = pl.pallas_call(
        fine_kernel,
        out_shape=(
            shape(count, depth + 4, *plane),
            shape(count, depth + 2, *plane),
            shape(count, depth + 2, *plane),
            shape(half + half // 2, rows1, LANES),
        ),
        in_specs=[SMEM, SMEM] + [VMEM] * 7,
        out_specs=(VMEM,) * 4,
        scratch_shapes=[
            scratch(count, depth + 2 * REACH, *plane),
            scratch(count, depth + 2 * REACH, *plane),
            scratch(half * count + half, *plane),
        ],
        compiler_params=params,
    )(level_shifts, assignment, near(own_scaled), near(own_weight), potential, low, high, up, down)

    gathered = lax.all_gather(payload, "dom", axis=0)

    window = 7 * half
    update = pl.pallas_call(
        coarse_kernel,
        out_shape=shape(count, depth, *plane),
        in_specs=[SMEM, SMEM, SMEM] + [VMEM] * 5,
        out_specs=VMEM,
        scratch_shapes=[
            scratch(window, rows1, LANES),
            scratch(window, rows1, LANES),
            scratch(window, rows1, LANES),
            scratch(window, rows1, LANES),
            scratch(2 * (window // 2 - 2), rows1, LANES),
            scratch(6, rows1, LANES),
            scratch(half + 6, rows1, LANES),
            scratch(half + 4, rows1, LANES),
            scratch(count, half + 2, *plane),
            scratch(count, depth + 4, *plane),
            scratch(count, depth + 2, *plane),
        ],
        compiler_params=params,
    )(place, level_shifts, assignment, gathered, estimate, scaled, weight, initial_guess)

    rows = (1 + len(blocks)) * count * count
    sums = pl.pallas_call(
        early_kernel,
        out_shape=shape(rows, LANES),
        in_specs=[VMEM] * (2 + len(blocks)),
        out_specs=VMEM,
        compiler_params=params,
    )(update, orbitals, *blocks)
    sums = pl.pallas_call(
        late_kernel,
        out_shape=shape(1, LANES),
        in_specs=[SMEM] + [VMEM] * (2 + len(last)),
        out_specs=VMEM,
        scratch_shapes=[scratch(rows + count * count, LANES)],
        compiler_params=params,
    )(outside, update, sums, *last)
    parts = reduce_parts(sums, "dom")
    cells = float(depth * members * ny * nz)
    return pl.pallas_call(
        functools.partial(project_kernel, len(blocks), len(parts), cells),
        out_shape=shape(count, depth, *plane),
        in_specs=[SMEM] + [VMEM] * (2 + len(blocks) + len(last) + len(parts)),
        out_specs=HBM,
        scratch_shapes=[scratch(count, depth, *plane), pltpu.SemaphoreType.DMA((depth,))],
        compiler_params=params,
    )(outside, update, orbitals, *blocks, *last, *parts)


def solution(mesh):
    in_specs = (
        P("orb", "dom", None, None),
        P("orb", "dom", None, None),
        P("dom", None, None),
        P("dom", None, None),
        P(),
        P("orb"),
    )
    return jax.shard_map(
        on_device,
        mesh=mesh,
        in_specs=in_specs,
        out_specs=P("orb", "dom", None, None),
        check_vma=False,
    )
```

```python
import functools

import jax
import jax.numpy as jnp
from jax import lax
from jax.experimental import pallas as pl
from jax.experimental.pallas import tpu as pltpu
from jax.sharding import PartitionSpec as P


OMEGA = 0.8
KINETIC = 8.0
LANES = 128
REACH = 3


F32 = jnp.float32
VMEM = pl.BlockSpec(memory_space=pltpu.VMEM)
SMEM = pl.BlockSpec(memory_space=pltpu.SMEM)
HBM = pl.BlockSpec(memory_space=pltpu.HBM)


def roll(x, shift, axis):
    return pltpu.roll(x, shift % x.shape[axis], axis)


def around(x, group):
    y, z = x.ndim - 2, x.ndim - 1
    total = roll(x, 1, y) + roll(x, -1, y)
    if group == x.shape[z]:
        return total + (roll(x, 1, z) + roll(x, -1, z))
    place = lax.broadcasted_iota(jnp.int32, x.shape, z) % group
    before = jnp.where(place == 0, roll(x, 1 - group, z), roll(x, 1, z))
    after = jnp.where(place == group - 1, roll(x, group - 1, z), roll(x, -1, z))
    return total + (before + after)


def exact_dot(values, table):
    high = values.astype(jnp.bfloat16)
    rest = values - high.astype(F32)
    middle = rest.astype(jnp.bfloat16)
    low = (rest - middle.astype(F32)).astype(jnp.bfloat16)
    dot = functools.partial(jnp.dot, preferred_element_type=F32)
    return dot(high, table) + (dot(middle, table) + dot(low, table))


def pair_table(rows, columns, value):
    r = lax.broadcasted_iota(jnp.int32, (rows, columns), 0)
    c = lax.broadcasted_iota(jnp.int32, (rows, columns), 1)
    return jnp.where(r // 2 == c, value, 0.0).astype(jnp.bfloat16)


def spread_table(rows, columns):
    r = lax.broadcasted_iota(jnp.int32, (rows, columns), 0)
    c = lax.broadcasted_iota(jnp.int32, (rows, columns), 1)
    return jnp.where(c // 2 == r, 1.0, 0.0).astype(jnp.bfloat16)


def load_all(pairs, sems):
    copies = [
        pltpu.make_async_copy(source, target, sems.at[k]) for k, (source, target) in enumerate(pairs)
    ]
    for copy in copies:
        copy.start()
    for copy in copies:
        copy.wait()


def own_source(i, x, constant, guess, orbital, potential, perturbation):
    value = guess[i, x]
    near = around(value, LANES)
    if x > 0:
        near = near + guess[i, x - 1]
    if x < guess.shape[1] - 1:
        near = near + guess[i, x + 1]
    return KINETIC * near - (constant + potential[x]) * value - perturbation[x] * orbital[i, x]


def edge_kernel(
    shifts_in, assigned_in, guess_in, orbital_in, potential_in, perturbation_in, up, down,
    shifts, assigned, guess, orbital, potential, perturbation, sems,
):
    fields = (guess, orbital, potential, perturbation)
    inputs = (shifts_in, assigned_in, guess_in, orbital_in, potential_in, perturbation_in)
    load_all(zip(inputs, (shifts, assigned) + fields), sems)
    count, depth = guess.shape[:2]
    for i in range(count):
        constant = 6.0 * KINETIC + shifts[assigned[i]]
        down[i] = guess[i, 0]
        up[i] = guess[i, depth - 1]
        for x in range(REACH):
            down[(1 + x) * count + i] = own_source(i, x, constant, *fields)
            up[(1 + x) * count + i] = own_source(i, depth - 1 - x, constant, *fields)
    for x in range(REACH):
        down[(1 + REACH) * count + x] = potential[x]
        up[(1 + REACH) * count + x] = potential[depth - 1 - x]


def own_kernel(
    shifts_in, assigned_in, guess_in, orbital_in, potential_in, perturbation_in, scaled, weight,
    shifts, assigned, guess, orbital, potential, perturbation, sems,
):
    fields = (guess, orbital, potential, perturbation)
    inputs = (shifts_in, assigned_in, guess_in, orbital_in, potential_in, perturbation_in)
    load_all(zip(inputs, (shifts, assigned) + fields), sems)
    count, depth = guess.shape[:2]
    for i in range(count):
        constant = 6.0 * KINETIC + shifts[assigned[i]]
        for x in range(depth):
            w = OMEGA / (constant + potential[x])
            weight[i, x] = KINETIC * w
            scaled[i, x] = w * own_source(i, x, constant, *fields)


def fine_kernel(
    shifts, assigned, own_scaled, own_weight, potential, low, high, up, down, estimate, scaled, weight, payload,
    all_scaled, all_weight, pairs,
):
    count, depth = own_scaled.shape[:2]
    planes = depth + 2 * REACH
    first = (1 + REACH) * count

    for i in range(count):
        constant = 6.0 * KINETIC + shifts[assigned[i]]
        for p in range(planes):
            x = p - REACH
            if 0 <= x < depth:
                kw = own_weight[i, x]
                g = own_scaled[i, x]
                if x == 0:
                    g = g + kw * low[i]
                if x == depth - 1:
                    g = g + kw * high[i]
            else:
                side, away = (low, -1 - x) if x < 0 else (high, x - depth)
                w = OMEGA / (constant + side[first + away])
                kw = KINETIC * w
                g = w * side[(1 + away) * count + i]
                if away == 0:
                    g = g + kw * (down if x < 0 else up)[i]
            all_weight[i, p] = kw
            all_scaled[i, p] = g
            if 2 <= p < planes - 2:
                scaled[i, p - 2] = g
                weight[i, p - 2] = kw
    for i in range(count):
        for p in range(1, planes - 1):
            g = all_scaled[i, p]
            near = around(g, LANES) + (all_scaled[i, p - 1] + all_scaled[i, p + 1])
            estimate[i, p - 1] = (2.0 - OMEGA) * g + all_weight[i, p] * near
    half = depth // 2
    for i in range(count):
        constant = 6.0 * KINETIC + shifts[assigned[i]]
        for q in range(half):
            total = None
            for x in (2 * q, 2 * q + 1):
                e = estimate[i, x + 2]
                near = around(e, LANES) + (estimate[i, x + 1] + estimate[i, x + 3])
                r = (constant + potential[x]) * (
                    (1.0 / OMEGA) * all_scaled[i, x + REACH] - e
                ) + KINETIC * near
                total = r if total is None else total + r
            pairs[q * count + i] = total
    for q in range(half):
        pairs[half * count + q] = potential[2 * q] + potential[2 * q + 1]
    rows = pairs.shape[1] // 2
    slots = pairs.shape[0] // 2
    even = pairs[:, pl.ds(0, rows, 2), :] + pairs[:, pl.ds(1, rows, 2), :]
    even = even.reshape(slots, 2, rows, LANES)
    both = jnp.concatenate([even[:, 0], even[:, 1]], axis=-1).reshape(slots * rows, 2 * LANES)
    payload[...] = exact_dot(both, pair_table(2 * LANES, LANES, 0.125)).reshape(slots, rows, LANES)


def coarse_kernel(
    place, shifts, assigned, gathered, estimate, scaled, weight, guess, update,
    scaled1, weight1, coef1, e1, pairs, spread2, a1, b1, spread1, a0, b0,
):
    members = gathered.shape[0]
    count, depth = guess.shape[:2]
    half = depth // 2
    reach = 3
    window = (2 * reach + 1) * half
    rows1 = gathered.shape[2]
    group1 = LANES // count
    k1 = KINETIC / 4
    k2 = KINETIC / 16

    def shift_lanes(group):
        lane = lax.broadcasted_iota(jnp.int32, (1, 1, LANES), 2) // group
        value = jnp.full((1, 1, LANES), shifts[assigned[0]], F32)
        for i in range(1, count):
            value = jnp.where(lane % count == i, shifts[assigned[i]], value)
        return value

    base1 = 6.0 * k1 + shift_lanes(group1)
    base2 = 6.0 * k2 + shift_lanes(group1 // 2)
    lane = lax.broadcasted_iota(jnp.int32, (1, rows1, LANES), 2)
    for s in range(2 * reach + 1):
        slot = lax.rem(place[0] + (s - reach + 2 * members), members)
        f = gathered[slot, 0:half]
        for t in range(half // 2):
            packed = gathered[slot, half + t : half + t + 1]
            swapped = roll(packed, LANES // 2, 2)
            coef1[s * half + 2 * t : s * half + 2 * t + 1] = jnp.where(
                lane < LANES // 2, packed, swapped
            )
            coef1[s * half + 2 * t + 1 : s * half + 2 * t + 2] = jnp.where(
                lane < LANES // 2, swapped, packed
            )
        w = OMEGA / (base1 + coef1[s * half : (s + 1) * half])
        weight1[s * half : (s + 1) * half] = k1 * w
        scaled1[s * half : (s + 1) * half] = w * f
    step = 4
    for p in range(1, window - 1, step):
        stop = min(p + step, window - 1)
        g = scaled1[p:stop]
        near = around(g, group1) + (scaled1[p - 1 : stop - 1] + scaled1[p + 1 : stop + 1])
        e1[p:stop] = (2.0 - OMEGA) * g + weight1[p:stop] * near
    coarse = window // 2 - 2
    for p in range(2, window - 2, step):
        stop = min(p + step, window - 2)
        e = e1[p:stop]
        near = around(e, group1) + (e1[p - 1 : stop - 1] + e1[p + 1 : stop + 1])
        c = coef1[p:stop]
        r = (base1 + c) * ((1.0 / OMEGA) * scaled1[p:stop] - e) + k1 * near
        for t in range(0, stop - p, 2):
            pairs[(p + t) // 2 - 1] = r[t] + r[t + 1]
            pairs[coarse + (p + t) // 2 - 1] = c[t] + c[t + 1]
    rows2 = rows1 // 2
    even = pairs[:, pl.ds(0, rows2, 2), :] + pairs[:, pl.ds(1, rows2, 2), :]
    both = exact_dot(
        even.reshape(2 * coarse * rows2, LANES), pair_table(LANES, LANES, 0.125)
    ).reshape(2 * coarse, rows2, LANES)
    w = OMEGA / (base2 + both[coarse:])
    g = w * both[:coarse]
    w = k2 * w
    e = None
    for _ in range(3):
        n = g.shape[0]
        if e is None:
            e = g
            mine = (2.0 - OMEGA) * g[1 : n - 1]
        else:
            mine = (1.0 - OMEGA) * e[1 : n - 1] + g[1 : n - 1]
        near = around(e[1 : n - 1], group1 // 2) + (e[0 : n - 2] + e[2:n])
        e = mine + w[1 : n - 1] * near
        g, w = g[1 : n - 1], w[1 : n - 1]
    n = e.shape[0]
    wide = exact_dot(e.reshape(n * rows2, LANES), spread_table(LANES, LANES))
    wide = wide.reshape(n, rows2, LANES)
    spread2[:, pl.ds(0, rows2, 2), :] = wide
    spread2[:, pl.ds(1, rows2, 2), :] = wide
    origin = reach * half
    for q in range(-3, half + 3):
        a1[q + 3] = e1[origin + q] + spread2[(q + 4) // 2]

    def sweep1(source, start, stop, offset):
        e = source[start - offset : stop - offset]
        near = around(e, group1) + (
            source[start - 1 - offset : stop - 1 - offset]
            + source[start + 1 - offset : stop + 1 - offset]
        )
        window = slice(origin + start, origin + stop)
        return (1.0 - OMEGA) * e + scaled1[window] + weight1[window] * near

    for q in range(-2, half + 2, 4):
        b1[q + 2 : q + 6] = sweep1(a1, q, q + 4, -3)
    last = sweep1(b1, -1, half + 1, -2)
    n = last.shape[0]
    wide = exact_dot(last.reshape(n * rows1, LANES), spread_table(LANES, count * LANES))
    wide = wide.reshape(n, rows1, count * LANES)
    for i in range(count):
        part = wide[:, :, i * LANES : (i + 1) * LANES]
        spread1[i, :, pl.ds(0, rows1, 2), :] = part
        spread1[i, :, pl.ds(1, rows1, 2), :] = part
    for i in range(count):
        for p in range(depth + 4):
            a0[i, p] = estimate[i, p] + spread1[i, p // 2]
    for i in range(count):
        for p in range(depth + 2):
            e = a0[i, p + 1]
            near = around(e, LANES) + (a0[i, p] + a0[i, p + 2])
            b0[i, p] = (1.0 - OMEGA) * e + scaled[i, p] + weight[i, p] * near
    for i in range(count):
        for p in range(depth):
            e = b0[i, p + 1]
            near = around(e, LANES) + (b0[i, p] + b0[i, p + 2])
            update[i, p] = guess[i, p] + (
                (1.0 - OMEGA) * e + scaled[i, p + 1] + weight[i, p + 1] * near
            )


def row_sums(blocks, update, out, first):
    count, depth, rows = update.shape[:3]

    def body(x, totals):
        totals = list(totals)
        u = [update[i, x].reshape(rows // 8, 8, LANES) for i in range(count)]
        for r, block in enumerate(blocks):
            for j in range(count):
                o = block(j, x).reshape(rows // 8, 8, LANES)
                for i in range(count):
                    totals[(r * count + j) * count + i] += jnp.sum(o * u[i], axis=0)
        return tuple(totals)

    zero = jnp.zeros((8, LANES), F32)
    totals = lax.fori_loop(0, depth, body, (zero,) * (len(blocks) * count * count))
    for k, total in enumerate(totals):
        out[first + k : first + k + 1] = jnp.sum(total, axis=0, keepdims=True)


def reader(ref, other=None, use_other=None):
    def read(j, x):
        if other is None:
            return ref[j, x]
        return jnp.where(use_other, other[j, x], ref[j, x])

    return read


def chosen(last, outside):
    return (outside[0] == 1,) if len(last) == 2 else ()


def early_kernel(update, own, *refs):
    row_sums([reader(ref) for ref in (own,) + refs[:-1]], update, refs[-1], 0)


def lane_of(rows):
    place = (rows, LANES)
    return lax.broadcasted_iota(jnp.int32, place, 0) == lax.broadcasted_iota(jnp.int32, place, 1)


def late_kernel(outside, update, early, *refs):
    last, (out, sums) = refs[:-2], refs[-2:]
    rows = early.shape[0]
    sums[0:rows] = early[...]
    row_sums([reader(*last, *chosen(last, outside))], update, sums, rows)
    total = jnp.sum(sums[...], axis=1, keepdims=True)
    out[...] = jnp.sum(jnp.where(lane_of(sums.shape[0]), total, 0.0), axis=0, keepdims=True)


def project_kernel(blocks, parts, cells, outside, update, own, *refs):
    others, last = refs[:blocks], refs[blocks : -3 - parts]
    sums, (out_ref, out, sems) = refs[-3 - parts : -3], refs[-3:]
    count, depth, _ = update.shape[:3]
    total = sums[0][...]
    for part in sums[1:]:
        total = total + part[...]
    pairs = (2 + blocks) * count * count
    spread = jnp.where(lane_of(pairs), jnp.broadcast_to(total, (pairs, LANES)), 0.0)
    overlap = jnp.sum(spread, axis=1, keepdims=True) / cells
    reads = [reader(ref) for ref in (own,) + others] + [reader(*last, *chosen(last, outside))]

    def store(i, x):
        return pltpu.make_async_copy(out.at[i, x], out_ref.at[i, x], sems.at[i, x])

    for x in range(depth):
        values = [update[i, x] for i in range(count)]
        for r, read in enumerate(reads):
            for j in range(count):
                o = read(j, x)
                for i in range(count):
                    k = (r * count + j) * count + i
                    values[i] = values[i] - overlap[k : k + 1] * o
        for i in range(count):
            out[i, x] = values[i]
            store(i, x).start()
    for x in range(depth):
        for i in range(count):
            store(i, x).wait()


def gather_blocks(block, axis):
    n = lax.axis_size(axis)
    if n == 4:
        first = lax.ppermute(block, axis, [(0, 2), (3, 1), (2, 3), (1, 0)])
        second = lax.ppermute(block, axis, [(1, 3), (2, 0), (0, 1), (3, 2)])
        inner = lax.ppermute(block, axis, [(1, 2), (2, 1), (0, 0), (3, 3)])
        outer = lax.ppermute(first, axis, [(2, 3), (1, 0), (0, 1), (3, 2)])
        return [first, second], [inner, outer]
    blocks = []
    for r in range(1, n):
        blocks.append(lax.ppermute(block, axis, [((i + r) % n, i) for i in range(n)]))
    return blocks[:-1], blocks[-1:]


def reduce_parts(value, axis):
    n = lax.axis_size(axis)
    if n & (n - 1):
        return [lax.psum(value, axis)]
    parts, top = [value], n
    while top > 1:
        total = parts[0]
        for part in parts[1:]:
            total = total + part
        width = min(4, top // 2) if top > 2 else 2
        top //= width
        parts = [total]
        for k in range(width - 1, 0, -1):
            pairs = [(i, i ^ (k * top)) for i in range(n)]
            parts.append(lax.ppermute(total, axis, pairs))
    return parts


def on_device(orbitals, initial_guess, potential, perturbation, level_shifts, assignment):
    count, depth, ny, nz = orbitals.shape
    near = lambda x: pltpu.with_memory_space_constraint(x, pltpu.HBM)
    members = lax.axis_size("dom")
    half, rows1 = depth // 2, ny // 2
    assert nz == LANES and count * (nz // 2) == LANES and depth >= 2 * REACH
    plane = (ny, nz)
    shape = lambda *dims: jax.ShapeDtypeStruct(dims, F32)
    scratch = lambda *dims: pltpu.VMEM(dims, F32)
    params = pltpu.CompilerParams(vmem_limit_bytes=24 * 1024 * 1024)
    place = lax.axis_index("dom").astype(jnp.int32).reshape(1)

    blocks, last = gather_blocks(orbitals, "orb")
    rank = lax.axis_index("orb")
    outside = jnp.logical_or(rank == 0, rank == lax.axis_size("orb") - 1).astype(jnp.int32).reshape(1)

    message = (1 + REACH) * count + REACH
    inputs = tuple(
        map(near, (level_shifts, assignment, initial_guess, orbitals, potential, perturbation))
    )
    local = [
        pltpu.SMEM(level_shifts.shape, F32),
        pltpu.SMEM(assignment.shape, jnp.int32),
        scratch(count, depth, *plane),
        scratch(count, depth, *plane),
        scratch(depth, *plane),
        scratch(depth, *plane),
        pltpu.SemaphoreType.DMA((6,)),
    ]
    up, down = pl.pallas_call(
        edge_kernel,
        out_shape=(shape(message, *plane),) * 2,
        in_specs=[HBM] * 6,
        out_specs=(VMEM,) * 2,
        scratch_shapes=local,
        compiler_params=params,
    )(*inputs)
    own_scaled, own_weight = pl.pallas_call(
        own_kernel,
        out_shape=(shape(count, depth, *plane),) * 2,
        in_specs=[HBM] * 6,
        out_specs=(VMEM,) * 2,
        scratch_shapes=local,
        compiler_params=params,
    )(*inputs)
    low = lax.ppermute(up, "dom", [(i, (i + 1) % members) for i in range(members)])
    high = lax.ppermute(down, "dom", [((i + 1) % members, i) for i in range(members)])

    estimate, scaled, weight, payload = pl.pallas_call(
        fine_kernel,
        out_shape=(
            shape(count, depth + 4, *plane),
            shape(count, depth + 2, *plane),
            shape(count, depth + 2, *plane),
            shape(half + half // 2, rows1, LANES),
        ),
        in_specs=[SMEM, SMEM] + [VMEM] * 7,
        out_specs=(VMEM,) * 4,
        scratch_shapes=[
            scratch(count, depth + 2 * REACH, *plane),
            scratch(count, depth + 2 * REACH, *plane),
            scratch(half * count + half, *plane),
        ],
        compiler_params=params,
    )(level_shifts, assignment, near(own_scaled), near(own_weight), potential, low, high, up, down)

    gathered = lax.all_gather(payload, "dom", axis=0)

    window = 7 * half
    update = pl.pallas_call(
        coarse_kernel,
        out_shape=shape(count, depth, *plane),
        in_specs=[SMEM, SMEM, SMEM] + [VMEM] * 5,
        out_specs=VMEM,
        scratch_shapes=[
            scratch(window, rows1, LANES),
            scratch(window, rows1, LANES),
            scratch(window, rows1, LANES),
            scratch(window, rows1, LANES),
            scratch(2 * (window // 2 - 2), rows1, LANES),
            scratch(6, rows1, LANES),
            scratch(half + 6, rows1, LANES),
            scratch(half + 4, rows1, LANES),
            scratch(count, half + 2, *plane),
            scratch(count, depth + 4, *plane),
            scratch(count, depth + 2, *plane),
        ],
        compiler_params=params,
    )(place, level_shifts, assignment, gathered, estimate, scaled, weight, initial_guess)

    rows = (1 + len(blocks)) * count * count
    sums = pl.pallas_call(
        early_kernel,
        out_shape=shape(rows, LANES),
        in_specs=[VMEM] * (2 + len(blocks)),
        out_specs=VMEM,
        compiler_params=params,
    )(update, orbitals, *blocks)
    sums = pl.pallas_call(
        late_kernel,
        out_shape=shape(1, LANES),
        in_specs=[SMEM] + [VMEM] * (2 + len(last)),
        out_specs=VMEM,
        scratch_shapes=[scratch(rows + count * count, LANES)],
        compiler_params=params,
    )(outside, update, sums, *last)
    parts = reduce_parts(sums, "dom")
    cells = float(depth * members * ny * nz)
    return pl.pallas_call(
        functools.partial(project_kernel, len(blocks), len(parts), cells),
        out_shape=shape(count, depth, *plane),
        in_specs=[SMEM] + [VMEM] * (2 + len(blocks) + len(last) + len(parts)),
        out_specs=HBM,
        scratch_shapes=[scratch(count, depth, *plane), pltpu.SemaphoreType.DMA((count, depth))],
        compiler_params=params,
    )(outside, update, orbitals, *blocks, *last, *parts)


def solution(mesh):
    in_specs = (
        P("orb", "dom", None, None),
        P("orb", "dom", None, None),
        P("dom", None, None),
        P("dom", None, None),
        P(),
        P("orb"),
    )
    return jax.shard_map(
        on_device,
        mesh=mesh,
        in_specs=in_specs,
        out_specs=P("orb", "dom", None, None),
        check_vma=False,
    )
```
